32 devices in a mesh: row: 4 (over z), col: 8 (over y, x, core).
Axes of the slice: x: 2, y: 2, z: 4, core: 2. Of those that a mesh axis runs over, the one named last changes fastest.
Arguments:
- residual: float32 [8192, 2048], P('row', 'col'), may hold values from -6 to 6
- point_spread: float32 [1024, 1024], P('col'), may hold values from -0.6 to 1
- peak_pixels: int32 [4, 64, 2], replicated, may hold values from 0 to 8191, as said below
Outputs:
- cleaned: float32 [8192, 2048], P('row', 'col')
- tile_peak: float32 [4, 8], P('row', 'col')
- components: float32 [4, 64], replicated
The draws below stay inside these ranges and needn't reach their ends.
Inputs may be any that keep to these rules, and one draw needn't show every extreme that they name: peak_pixels[r, k, 0] is a row below 8192 and peak_pixels[r, k, 1] a column below 2048; positions may repeat.
All inputs are finite; a program needn't handle non-finite values.
Results may differ from the reference program's by a relative error of at most 0.00002.
Values sent between devices are 32-bit elements; how exact they have to be, the bound alone decides.
A program may use at most 64 MiB of HBM per device.

```python
import jax
import jax.numpy as jnp
from jax import lax

PS = 1024
PEAKS = 64
ROUNDS = 4
TR = 2048
TC = 256
NR = 8192
NC = 2048
N_ROW = 4
N_COL = 8


def draw_point_spread(key, part):
    axis_pos = jnp.arange(PS, dtype=jnp.float32) - PS // 2
    radius = axis_pos[:, None] ** 2 + axis_pos[None, :] ** 2
    bump_width = PS / 64.0
    central = jnp.exp(-radius / (2.0 * bump_width * bump_width))
    sidelobes = jnp.clip(0.15 * jax.random.normal(key, (PS, PS), jnp.float32), -0.6, 0.6)
    return central + sidelobes * (1.0 - central)


def draw_peak_pixels(key, part):
    cluster_count = PEAKS * 3 // 16
    subkeys = jax.random.split(key, 6)
    flat_rows = jax.random.randint(subkeys[0], (ROUNDS, PEAKS), 0, NR)
    flat_cols = jax.random.randint(subkeys[1], (ROUNDS, PEAKS), 0, NC)
    centre_rows = jax.random.randint(subkeys[2], (ROUNDS, 1), 0, NR)
    centre_cols = jax.random.randint(subkeys[3], (ROUNDS, 1), 0, NC)
    jitter_rows = jax.random.randint(subkeys[4], (ROUNDS, PEAKS), -PS, PS + 1)
    jitter_cols = jax.random.randint(subkeys[5], (ROUNDS, PEAKS), -(PS // 4), PS // 4 + 1)
    near_rows = jnp.clip(centre_rows + jitter_rows, 0, NR - 1)
    near_cols = jnp.clip(centre_cols + jitter_cols, 0, NC - 1)
    is_cluster = jnp.arange(PEAKS)[None, :] < cluster_count
    row_pixels = jnp.where(is_cluster, near_rows, flat_rows)
    col_pixels = jnp.where(is_cluster, near_cols, flat_cols)
    return jnp.stack([row_pixels, col_pixels], axis=2).astype(jnp.int32)


def shard_levels(rng, dims, shards, least, largest):
    gain = 1.0
    for dim, shards_of in shards:
        draws = jax.random.uniform(jax.random.fold_in(jax.random.fold_in(rng, 6), dim), (shards_of,), jnp.float32, least / len(shards), largest / len(shards))
        gain = gain * jnp.repeat(jnp.exp(draws), dims[dim] // shards_of).reshape((-1,) + (1,) * (len(dims) - 1 - dim))
    return gain


def scatter_about(stream_key, dims, width, limit, shards=(), kind=jnp.bfloat16):
    values = width * jax.random.normal(stream_key, dims, jnp.float32)
    if shards:
        values = values * shard_levels(stream_key, dims, shards, -0.22, 0.18)
    return jnp.clip(values, -limit, limit).astype(kind)


def setup_inputs(seed: int = 0) -> dict:
    splits = jax.random.split(jax.random.key(seed), 4)
    return {
        "residual": scatter_about(splits[0], (NR, NC), 1.0, 6.0, ((0, 4), (1, 8)), jnp.float32),
        "point_spread": draw_point_spread(jax.random.fold_in(splits[3], 71), 0),
        "peak_pixels": draw_peak_pixels(jax.random.fold_in(splits[3], 71), 0),
    }


loop_gain = 0.1


def reference(residual, point_spread, peak_pixels):
    half_width = PS // 2
    canvas = jnp.pad(residual, ((PS, PS), (PS, PS)))
    amplitude_rows = []
    for round_index in range(ROUNDS):
        peak_rows = peak_pixels[round_index, :, 0].astype(jnp.int32)
        peak_cols = peak_pixels[round_index, :, 1].astype(jnp.int32)
        values = canvas[peak_rows + PS, peak_cols + PS]
        amplitudes = loop_gain * values
        amplitude_rows.append(amplitudes)

        def subtract(position, current):
            first_row = (peak_rows[position] + half_width).astype(jnp.int32)
            first_col = (peak_cols[position] + half_width).astype(jnp.int32)
            window = lax.dynamic_slice(current, (first_row, first_col), (PS, PS))
            return lax.dynamic_update_slice(current, window - amplitudes[position] * point_spread, (first_row, first_col))

        canvas = lax.fori_loop(0, PEAKS, subtract, canvas)
    cleaned = canvas[PS:PS + NR, PS:PS + NC]
    tile_peak = jnp.max(jnp.abs(cleaned).reshape(N_ROW, TR, N_COL, TC), axis=(1, 3))
    return cleaned, tile_peak, jnp.stack(amplitude_rows)
```

```python
import functools

import jax
import jax.numpy as jnp
from jax import lax
from jax.experimental import pallas as pl
from jax.experimental.pallas import tpu as pltpu
from jax.sharding import PartitionSpec as P

loop_gain = 0.1
LANES = 128
LINE_BIT = 7
CHUNK_BIT = 24
LINE_MASK = (1 << (CHUNK_BIT - LINE_BIT)) - 1
MESH = pl.DeviceIdType.MESH
PAD = 64
AHEAD = 4
SCRATCH = 24 << 20


def gather_kernel(
    n_row, n_col, rows_done, rounds, peaks,
    code_ref, psf_ref, res_ref,
    beam, table_out,
    image, load_sem, image_sem,
    send_sem, recv_sem, pair_send, small_send, small_recv,
):
    n_dev = n_row * n_col
    side = psf_ref.shape[1]
    chunks = side // LANES
    edge = (beam.shape[0] - chunks) // 2
    depth = side // n_col
    total = rounds * peaks
    groups = total // LANES
    row = lax.axis_index("row")
    col = lax.axis_index("col")
    me = row * n_col + col
    halves = 2
    half = chunks // halves

    def region(block, part):
        return beam.at[pl.ds(edge + part * half, half), pl.ds(PAD + block * depth, depth), :]

    own_loads = [
        pltpu.make_async_copy(
            psf_ref.at[:, pl.ds(c * LANES, LANES)],
            beam.at[edge + c, pl.ds(PAD + col * depth, depth), :],
            load_sem.at[c],
        )
        for c in range(chunks)
    ]
    for copy in own_loads:
        copy.start()
    tile_rows, tile_cols = res_ref.shape
    parts = tile_cols // LANES
    image_loads = [
        pltpu.make_async_copy(
            res_ref.at[:, pl.ds(u * LANES, LANES)], image.at[u], image_sem.at[u]
        )
        for u in range(parts)
    ]
    for copy in image_loads:
        copy.start()

    frame = jnp.zeros((PAD, LANES), jnp.float32)
    for c in range(chunks):
        beam[edge + c, pl.ds(0, PAD), :] = frame
        beam[edge + c, pl.ds(PAD + side, PAD), :] = frame

    def blank(step, _):
        at = pl.multiple_of(step * PAD, PAD)
        for c in list(range(edge)) + list(range(edge + chunks, 2 * edge + chunks)):
            beam[c, pl.ds(at, PAD), :] = frame
        return 0

    lax.fori_loop(0, side // PAD + 2, blank, 0)
    image[parts, pl.ds(0, 8), :] = jnp.zeros((8, LANES), jnp.float32)
    barrier = pltpu.get_barrier_semaphore()

    def greet(offset, _):
        other = lax.rem(me + offset, n_dev)
        pl.semaphore_signal(
            barrier, inc=1, device_id=(other // n_col, lax.rem(other, n_col)), device_id_type=MESH
        )
        return 0

    lax.fori_loop(1, n_dev, greet, 0)
    for copy in own_loads:
        copy.wait()
    pl.semaphore_wait(barrier, n_dev - 1)

    def send(block, part, target, slot):
        return pltpu.make_async_remote_copy(
            src_ref=region(block, part),
            dst_ref=region(block, part),
            send_sem=send_sem.at[slot],
            recv_sem=recv_sem.at[block, part],
            device_id=(row, target),
            device_id_type=MESH,
        )

    def to_partner(block):
        partner = col + 1 - 2 * lax.rem(col, 2)
        return [
            pltpu.make_async_remote_copy(
                src_ref=region(block, part),
                dst_ref=region(block, part),
                send_sem=pair_send.at[block // 2, part],
                recv_sem=recv_sem.at[block, part],
                device_id=(row, partner),
                device_id_type=MESH,
            )
            for part in range(halves)
        ]

    started = []

    def go(copy):
        copy.start()
        started.append(copy)

    if n_col == 8:
        bit_b = lax.rem(col // 2, 2)
        bit_a = col // 4
        near = col + 2 - 4 * bit_b
        far = col + 4 - 8 * bit_a
        across = near + 4 - 8 * bit_a
        go(send(col, 0, near, 0))
        go(send(col, 1, far, 1))
        go(send(col, 1, near, 2))
        go(send(col, 0, far, 3))
        own_pair = to_partner(col)
        near_pair, far_pair, across_pair = to_partner(near), to_partner(far), to_partner(across)
        go(own_pair[0])
        go(own_pair[1])
        send(near, 0, near, 0).wait_recv()
        go(send(near, 0, far, 4))
        go(near_pair[0])
        send(far, 1, far, 1).wait_recv()
        go(send(far, 1, near, 5))
        go(far_pair[1])
        send(near, 1, near, 2).wait_recv()
        go(near_pair[1])
        send(far, 0, far, 3).wait_recv()
        go(far_pair[0])
    else:
        chips = n_col // 2
        for step in range(1, chips):
            target = lax.rem(col + 2 * step, n_col)
            for part in range(halves):
                go(send(col, part, target, 2 * step + part))
        for copy in to_partner(col):
            go(copy)

    def pick(position, carry):
        lane = lax.broadcasted_iota(jnp.int32, (8, LANES), 1)
        code = code_ref[len(rows_done) * total + position]
        which = position & (LANES - 1)
        line = image[code >> CHUNK_BIT, pl.ds((code >> LINE_BIT) & LINE_MASK, 1), :]
        moved = pltpu.roll(jnp.broadcast_to(line, (8, LANES)), code & (LANES - 1), 1)
        return jnp.where(lane == which, moved, carry)

    for copy in image_loads:
        copy.wait()
    zero = jnp.zeros((8, LANES), jnp.float32)
    sublane = lax.broadcasted_iota(jnp.int32, (8, LANES), 0)
    picked = []
    for g in range(groups):
        found = lax.fori_loop(g * LANES, (g + 1) * LANES, pick, zero, unroll=32)
        picked.append(jnp.where(sublane == len(rows_done), found, 0.0))

    if n_col == 8:
        send(across, 0, far, 4).wait_recv()
        go(across_pair[0])
        send(across, 1, near, 5).wait_recv()
        go(across_pair[1])
    else:
        for step in range(1, chips):
            source = lax.rem(col - 2 * step + n_col, n_col)
            for part in range(halves):
                send(source, part, source, 0).wait_recv()
            for copy in to_partner(source):
                go(copy)
    parity = lax.rem(col, 2)
    for chip in range(n_col // 2):
        block = 2 * chip + 1 - parity
        for part in range(halves):
            send(block, part, col + 1 - 2 * parity, 0).wait_recv()

    for g in range(groups):
        active = [(t, need) for t, need in enumerate(rows_done) if need > g * LANES]
        bounds = sorted({min(need, (g + 1) * LANES) for _, need in active})
        carry = zero
        start = g * LANES
        for stop in bounds:
            live = [t for t, need in active if min(need, (g + 1) * LANES) >= stop]

            def look(position, acc):
                lane = lax.broadcasted_iota(jnp.int32, (8, LANES), 1)
                here = lane == (position & (LANES - 1))
                for t in live:
                    code = code_ref[t * total + position]
                    line = beam[code >> CHUNK_BIT, pl.ds((code >> LINE_BIT) & LINE_MASK, 1), :]
                    moved = pltpu.roll(jnp.broadcast_to(line, (8, LANES)), code & (LANES - 1), 1)
                    acc = jnp.where(here & (sublane == t), moved, acc)
                return acc

            carry = lax.fori_loop(start, stop, look, carry, unroll=16)
            start = stop
        table_out[me, pl.ds(g * 8, 8), :] = carry + picked[g]

    def small(offset, target, slot):
        return pltpu.make_async_remote_copy(
            src_ref=table_out.at[slot],
            dst_ref=table_out.at[slot],
            send_sem=small_send.at[offset],
            recv_sem=small_recv.at[offset],
            device_id=(target // n_col, lax.rem(target, n_col)),
            device_id_type=MESH,
        )

    def spread(offset, _):
        small(offset, lax.rem(me + offset, n_dev), me).start()
        return 0

    lax.fori_loop(1, n_dev, spread, 0)
    for copy in started:
        copy.wait_send()

    def collect(offset, _):
        other = lax.rem(me - offset + n_dev, n_dev)
        small(offset, other, other).wait_recv()
        small(offset, other, me).wait_send()
        return 0

    lax.fori_loop(1, n_dev, collect, 0)


def to_sublanes(line):
    square = lax.broadcasted_iota(jnp.int32, (LANES, LANES), 0) == lax.broadcasted_iota(
        jnp.int32, (LANES, LANES), 1
    )
    pieces = [
        jnp.sum(jnp.where(square, line[:, g : g + LANES], 0.0), axis=1, keepdims=True)
        for g in range(0, line.shape[1], LANES)
    ]
    return jnp.concatenate(pieces, axis=0)


def subtract_kernel(
    n_dev, skip, coeff_rows, rounds, peaks, side,
    pixel_ref, res_ref, beam_ref, table_ref,
    clean_ref, peak_ref, amp_ref,
    image, whole_line, real_line, whole_list, real_list,
    image_sem, store_sem, whole_sem, real_sem,
):
    tile_rows, tile_cols = clean_ref.shape
    pitch_rows = side + 2 * PAD
    parts = tile_cols // LANES
    total = rounds * peaks
    groups = total // LANES
    pitch = groups * 8
    blocks = tile_rows // PAD

    load = pltpu.make_async_copy(res_ref, image, image_sem)
    load.start()
    row_shift = lax.axis_index("row") * tile_rows + side // 2
    col_shift = lax.axis_index("col") * tile_cols + side // 2

    values = []
    for g in range(groups):
        part = table_ref[pl.ds(g * 8 + coeff_rows, n_dev, stride=pitch), :]
        values.append(jnp.sum(part, axis=0, keepdims=True))
    lane = lax.broadcasted_iota(jnp.int32, (1, LANES), 1)
    amps = [jnp.zeros((1, LANES), jnp.float32) for _ in range(groups)]
    piece = min(n_dev, peaks)
    for r in range(rounds):
        g_here = r * peaks // LANES
        lane_here = r * peaks % LANES
        taken = jnp.zeros((1, LANES), jnp.float32)
        if r:
            for first in range(r * peaks, (r + 1) * peaks, piece):
                device, slot = first % n_dev, first // n_dev - skip
                dots = jnp.zeros((piece, LANES), jnp.float32)
                for g in range((r * peaks + LANES - 1) // LANES):
                    rows = table_ref[pl.ds(device * pitch + g * 8 + slot, piece, stride=pitch), :]
                    dots = dots + rows * amps[g]
                sums = jnp.sum(dots, axis=1, keepdims=True)
                spot = lax.broadcasted_iota(jnp.int32, (piece, LANES), 0) + first % LANES
                diag = spot == lax.broadcasted_iota(jnp.int32, (piece, LANES), 1)
                taken = taken + jnp.sum(jnp.where(diag, sums, 0.0), axis=0, keepdims=True)
        fresh = loop_gain * (values[g_here] - taken)
        mine = (lane >= lane_here) & (lane < lane_here + peaks)
        amps[g_here] = jnp.where(mine, fresh, amps[g_here])
        amp_ref[pl.ds(r, 1), :] = fresh[:, lane_here : lane_here + peaks]

    far = 4.0 * tile_rows
    top = (pixel_ref[coeff_rows + 1 : coeff_rows + 2, :] - row_shift).astype(jnp.float32)
    left = (col_shift - pixel_ref[coeff_rows + 2 : coeff_rows + 3, :]).astype(jnp.float32)
    inside = (top > -side) & (top < tile_rows) & (left > -tile_cols) & (left < side)
    top = jnp.where(inside, top, far)
    index = lax.broadcasted_iota(jnp.int32, (1, total), 1).astype(jnp.float32)
    key = top * total + index
    key_down = to_sublanes(key)
    rank = jnp.sum(jnp.where(key < key_down, 1.0, 0.0), axis=1, keepdims=True)
    place = rank.astype(jnp.int32) == lax.broadcasted_iota(jnp.int32, (total, total), 1)
    top_down = to_sublanes(top)

    def ordered(down):
        return jnp.sum(jnp.where(place, down, 0.0), axis=0, keepdims=True)

    tops = ordered(top_down).astype(jnp.int32)
    lefts = ordered(to_sublanes(left)).astype(jnp.int32) + tile_cols
    lefts = jnp.clip(lefts, 0, side + tile_cols - 1)
    bound = lax.broadcasted_iota(jnp.int32, (1, LANES), 1)
    bound = jnp.where(bound < blocks, bound * PAD + PAD, (bound - blocks) * PAD - side + 1)
    count = jnp.sum(
        jnp.where(top_down < bound.astype(jnp.float32), 1.0, 0.0), axis=0, keepdims=True
    )
    spare = jnp.full((1, LANES), 4 * tile_rows, jnp.int32)
    whole_line[0:1, :total] = tops
    whole_line[0:1, total:] = spare
    whole_line[1:2, :total] = (lefts >> LINE_BIT) * pitch_rows + PAD
    whole_line[1:2, total:] = jnp.full((1, LANES), PAD, jnp.int32)
    whole_line[2:3, :total] = lefts & (LANES - 1)
    whole_line[2:3, total:] = jnp.zeros((1, LANES), jnp.int32)
    whole_line[3:4, :LANES] = count.astype(jnp.int32)
    real_line[0:1, :total] = ordered(to_sublanes(jnp.concatenate(amps, axis=1)))
    real_line[0:1, total:] = jnp.zeros((1, LANES), jnp.float32)
    copies = [
        pltpu.make_async_copy(whole_line, whole_list, whole_sem),
        pltpu.make_async_copy(real_line, real_list, real_sem),
    ]
    for copy in copies:
        copy.start()
    for copy in copies:
        copy.wait()
    load.wait()

    def store(block):
        at = pl.multiple_of(block * PAD, PAD)
        return pltpu.make_async_copy(
            image.at[pl.ds(at, PAD), :], clean_ref.at[pl.ds(at, PAD), :], store_sem.at[block]
        )

    lanes = lax.broadcasted_iota(jnp.int32, (PAD, LANES), 1)

    def settle(block, best):
        at = pl.multiple_of(block * PAD, PAD)
        begin, end = whole_list[3, blocks + block], whole_list[3, block]

        def several(step, held):
            held = list(held)
            for u in range(AHEAD):
                entry = begin + step * AHEAD + u
                offset = jnp.maximum(at - whole_list[0, entry], -PAD)
                first = whole_list[1, entry] + offset
                shift = whole_list[2, entry]
                amplitude = real_list[0, entry]
                turn = (LANES - shift) & (LANES - 1)
                keep = lanes >= shift
                cells = [
                    beam_ref[pl.ds(first + q * pitch_rows, PAD), :] for q in range(parts + 1)
                ]
                for q in range(parts):
                    moved = pltpu.roll(jnp.where(keep, cells[q], cells[q + 1]), turn, 1)
                    held[q] = held[q] - amplitude * moved
            return tuple(held)

        held = tuple(image[pl.ds(at, PAD), q * LANES : (q + 1) * LANES] for q in range(parts))
        held = lax.fori_loop(0, (end - begin + AHEAD - 1) // AHEAD, several, held)
        for q in range(parts):
            image[pl.ds(at, PAD), q * LANES : (q + 1) * LANES] = held[q]
            for i in range(0, PAD, 8):
                best = jnp.maximum(best, jnp.abs(held[q][i : i + 8, :]))
        store(block).start()
        return best

    best = lax.fori_loop(0, blocks, settle, jnp.zeros((8, LANES), jnp.float32))
    peak_ref[...] = jnp.max(jnp.max(best, axis=0, keepdims=True), axis=1, keepdims=True)

    def finish(block, _):
        store(block).wait()
        return 0

    lax.fori_loop(0, blocks, finish, 0)


def local(n_row, n_col, residual, point_spread, peak_pixels):
    n_dev = n_row * n_col
    tile_rows, tile_cols = residual.shape
    side = point_spread.shape[1]
    chunks = side // LANES
    half_width = side // 2
    rounds, peaks, _ = peak_pixels.shape
    total = rounds * peaks
    groups = total // LANES
    row_base = lax.axis_index("row") * tile_rows
    col_base = lax.axis_index("col") * tile_cols
    me = lax.axis_index("row") * n_col + lax.axis_index("col")

    per_device = total // n_dev
    skip = peaks // n_dev if peaks % n_dev == 0 else 0
    coeff_rows = per_device - skip
    if peaks % n_dev == 0:
        rows_done = tuple((t * n_dev // peaks) * peaks for t in range(skip, per_device))
    else:
        rows_done = (total,) * coeff_rows
    parts = tile_cols // LANES

    flat = peak_pixels.reshape(total, 2)
    prow, pcol = flat[:, 0], flat[:, 1]
    index = jnp.arange(total, dtype=jnp.int32)
    slots = lax.dynamic_slice(
        peak_pixels.reshape(per_device, n_dev, 2), (skip, me, 0), (coeff_rows, 1, 2)
    )
    target = me + n_dev * (jnp.arange(coeff_rows, dtype=jnp.int32) + skip)
    di = slots[:, :, 0] - prow[None, :] + half_width
    dj = slots[:, :, 1] - pcol[None, :] + half_width
    earlier = (index // peaks)[None, :] < (target // peaks)[:, None]
    valid = (di >= 0) & (di < side) & (dj >= 0) & (dj < side) & earlier
    look = (dj // LANES + parts << CHUNK_BIT) + (di + PAD << LINE_BIT)
    look = jnp.where(valid, look + (index[None, :] - dj) % LANES, 0)
    lr, lc = prow - row_base, pcol - col_base
    own = (lr >= 0) & (lr < tile_rows) & (lc >= 0) & (lc < tile_cols)
    pick = (lc // LANES << CHUNK_BIT) + (lr << LINE_BIT) + (index - lc) % LANES
    pick = jnp.where(own, pick, parts << CHUNK_BIT)
    codes = jnp.stack([*look, pick, prow, pcol])

    smem = pl.BlockSpec(memory_space=pltpu.SMEM)
    vmem = pl.BlockSpec(memory_space=pltpu.VMEM)
    hbm = pl.BlockSpec(memory_space=pltpu.HBM)
    dma = pltpu.SemaphoreType.DMA
    padded = (chunks + 2 * parts, side + 2 * PAD, LANES)
    beam, table = pl.pallas_call(
        functools.partial(gather_kernel, n_row, n_col, rows_done, rounds, peaks),
        out_shape=(
            pltpu.VMEM(padded, jnp.float32),
            pltpu.VMEM((n_dev, groups * 8, LANES), jnp.float32),
        ),
        in_specs=[smem, hbm, hbm],
        out_specs=(vmem, vmem),
        scratch_shapes=[
            pltpu.VMEM((parts + 1, tile_rows, LANES), jnp.float32),
            dma((chunks,)),
            dma((parts,)),
            dma((max(6, n_col),)),
            dma((n_col, 2)),
            dma((n_col // 2, 2)),
            dma((n_dev,)),
            dma((n_dev,)),
        ],
        compiler_params=pltpu.CompilerParams(
            collective_id=0, has_side_effects=True, vmem_limit_bytes=SCRATCH
        ),
        name="gather_beam",
    )(
        codes.reshape(-1),
        pltpu.with_memory_space_constraint(point_spread, pltpu.HBM),
        pltpu.with_memory_space_constraint(residual, pltpu.HBM),
    )

    cleaned, tile_peak, amps = pl.pallas_call(
        functools.partial(subtract_kernel, n_dev, skip, coeff_rows, rounds, peaks, side),
        out_shape=(
            jax.ShapeDtypeStruct((tile_rows, tile_cols), jnp.float32),
            jax.ShapeDtypeStruct((1, 1), jnp.float32),
            jax.ShapeDtypeStruct((rounds, peaks), jnp.float32),
        ),
        in_specs=[vmem, hbm, vmem, vmem],
        out_specs=(hbm, vmem, vmem),
        scratch_shapes=[
            pltpu.VMEM((tile_rows, tile_cols), jnp.float32),
            pltpu.VMEM((4, total + LANES), jnp.int32),
            pltpu.VMEM((1, total + LANES), jnp.float32),
            pltpu.SMEM((4, total + LANES), jnp.int32),
            pltpu.SMEM((1, total + LANES), jnp.float32),
            dma,
            dma((tile_rows // PAD,)),
            dma,
            dma,
        ],
        compiler_params=pltpu.CompilerParams(vmem_limit_bytes=SCRATCH),
        name="subtract",
    )(
        codes,
        residual,
        beam.reshape(padded[0] * padded[1], LANES),
        table.reshape(n_dev * groups * 8, LANES),
    )
    return cleaned, tile_peak, amps


def solution(mesh):
    return jax.shard_map(
        functools.partial(local, mesh.shape["row"], mesh.shape["col"]),
        mesh=mesh,
        in_specs=(P("row", "col"), P("col", None), P()),
        out_specs=(P("row", "col"), P("row", "col"), P()),
        check_vma=False,
    )
```

```python
import functools

import jax
import jax.numpy as jnp
from jax import lax
from jax.experimental import pallas as pl
from jax.experimental.pallas import tpu as pltpu
from jax.sharding import PartitionSpec as P

loop_gain = 0.1
LANES = 128
LINE_BIT = 7
CHUNK_BIT = 24
LINE_MASK = (1 << (CHUNK_BIT - LINE_BIT)) - 1
MESH = pl.DeviceIdType.MESH
PAD = 64
AHEAD = 8
STRIDE = 4
FRONT = 28
GROUP = 7
PIECES = 8
LAG = 2
LOADS = 2
SCRATCH = 11 << 20


def to_sublanes(line):
    square = lax.broadcasted_iota(jnp.int32, (LANES, LANES), 0) == lax.broadcasted_iota(
        jnp.int32, (LANES, LANES), 1
    )
    pieces = [
        jnp.sum(jnp.where(square, line[:, g : g + LANES], 0.0), axis=1, keepdims=True)
        for g in range(0, line.shape[1], LANES)
    ]
    return jnp.concatenate(pieces, axis=0)


def lane_iota(rows):
    return lax.broadcasted_iota(jnp.int32, (rows, LANES), 1)


def make_lists(row, col, tile_rows, tile_cols, side, pixels, lists, front):
    total = pixels.shape[1]
    spare = lists.shape[1] - total
    blocks = tile_rows // PAD
    pitch = side + 2 * PAD
    top = (pixels[0:1, :] - (row * tile_rows + side // 2)).astype(jnp.float32)
    left = (col * tile_cols + side // 2 - pixels[1:2, :]).astype(jnp.float32)
    inside = (top > -side) & (top < tile_rows) & (left > -tile_cols) & (left < side)
    start = jnp.clip(left.astype(jnp.int32) + tile_cols, 0, side + tile_cols - 1)
    height = jnp.minimum(top + side, tile_rows) - jnp.maximum(top, 0.0)
    height = jnp.where(inside, height, 0.0)
    index = lax.broadcasted_iota(jnp.int32, (1, total), 1).astype(jnp.float32)
    index_down = lax.broadcasted_iota(jnp.int32, (total, 1), 0).astype(jnp.float32)
    slot_at = lax.broadcasted_iota(jnp.int32, (total, total), 1).astype(jnp.float32)
    none, huge = -1.0, 1e9

    tall = index - height * total
    tall_down = to_sublanes(tall)
    rank_down = jnp.sum(jnp.where(tall < tall_down, 1.0, 0.0), axis=1, keepdims=True)
    rank = jnp.sum(jnp.where(tall_down < tall, 1.0, 0.0), axis=0, keepdims=True)
    in_down = to_sublanes(jnp.where(inside, 1.0, 0.0))
    chunk_down = to_sublanes((start >> LINE_BIT).astype(jnp.float32))
    shift_down = to_sublanes((start & (LANES - 1)).astype(jnp.float32))
    top_down = to_sublanes(top)

    def ordered(place_down, down, fill):
        picked = jnp.where(place_down == slot_at, down - fill, 0.0)
        return (jnp.sum(picked, axis=0, keepdims=True) + fill).astype(jnp.int32)

    last = (side + tile_cols - 1) >> LINE_BIT
    front[0:1, :] = jnp.clip(ordered(rank_down, chunk_down, 0.0), 0, last)
    front[1:2, :] = ordered(rank_down, shift_down, 0.0) & (LANES - 1)

    far = 4.0 * tile_rows
    by_top = top * total + index
    by_top_down = to_sublanes(by_top)
    bound = lane_iota(1)
    bound = jnp.where(bound < blocks, bound * PAD + PAD, (bound - blocks) * PAD - side + 1)
    bound = bound.astype(jnp.float32)
    line = 0
    for early in (True, False):
        chosen = inside & ((rank < FRONT) if early else (rank >= FRONT))
        side_down = (rank_down < FRONT) if early else (rank_down >= FRONT)
        chosen_down = jnp.where(side_down, in_down, 0.0)
        key = jnp.where(chosen, by_top, huge)
        place = jnp.sum(jnp.where(key < by_top_down, 1.0, 0.0), axis=1, keepdims=True)
        place = jnp.where(chosen_down > 0.0, place, none)
        if early:
            columns = [(top_down, far), (rank_down * (side + PAD) + PAD, PAD), (index_down, 0.0)]
        else:
            columns = [
                (top_down, far), (chunk_down * pitch + PAD, PAD),
                (index_down, 0.0), (shift_down, 0.0),
            ]
        for down, fill in columns:
            lists[line : line + 1, :total] = ordered(place, down, fill)
            lists[line : line + 1, total:] = jnp.full((1, spare), int(fill), jnp.int32)
            line += 1
        below = jnp.where(top_down < bound, chosen_down, 0.0)
        count = jnp.sum(below, axis=0, keepdims=True).astype(jnp.int32)
        at = 0 if early else LANES
        lists[7:8, at : at + LANES] = count


def gather_kernel(
    n_row, n_col, skip, rows_done, rounds, peaks,
    code_ref, pixel_ref, psf_ref, res_ref,
    beam, lists, amp_out, *rest,
):
    parts = res_ref.shape[1] // LANES
    rolled = rest[:parts]
    (
        image, front, front_list, table, load_sem, image_sem, front_sem,
        send_sem, recv_sem, pair_send, pair_recv, small_send, small_recv,
    ) = rest[parts:]
    n_dev = n_row * n_col
    side = psf_ref.shape[1]
    chunks = side // LANES
    edge = (beam.shape[0] - chunks) // 2
    depth = side // n_col
    total = rounds * peaks
    groups = total // LANES
    row = lax.axis_index("row")
    col = lax.axis_index("col")
    me = row * n_col + col
    tile_rows, tile_cols = res_ref.shape

    own_loads = [
        pltpu.make_async_copy(
            psf_ref.at[:, pl.ds(c * LANES, LANES)],
            beam.at[edge + c, pl.ds(PAD + col * depth, depth), :],
            load_sem.at[c],
        )
        for c in range(chunks)
    ]
    for copy in own_loads:
        copy.start()
    image_loads = [
        pltpu.make_async_copy(
            res_ref.at[:, pl.ds(u * LANES, LANES)], image.at[u], image_sem.at[u]
        )
        for u in range(parts)
    ]
    for copy in image_loads:
        copy.start()

    barrier = pltpu.get_barrier_semaphore()

    def greet(offset, _):
        other = lax.rem(me + offset, n_dev)
        pl.semaphore_signal(
            barrier, inc=1, device_id=(other // n_col, lax.rem(other, n_col)), device_id_type=MESH
        )
        return 0

    lax.fori_loop(1, n_dev, greet, 0)
    for copy in own_loads:
        copy.wait()
    pl.semaphore_wait(barrier, n_dev - 1)

    def remote(block, device, send, recv):
        region = beam.at[pl.ds(edge, chunks), pl.ds(PAD + block * depth, depth), :]
        return pltpu.make_async_remote_copy(
            src_ref=region,
            dst_ref=region,
            send_sem=send,
            recv_sem=recv,
            device_id=device,
            device_id_type=MESH,
        )

    started = []

    def go(copy):
        copy.start()
        started.append(copy)

    partner = (row, col + 1 - 2 * lax.rem(col, 2))
    chips = n_col // 2

    def hop(step, block):
        target = (row, lax.rem(col + 2 * step, n_col))
        return remote(block, target, send_sem.at[step], recv_sem.at[step])

    def pair(step, block):
        return remote(block, partner, pair_send.at[step], pair_recv.at[step])

    for step in range(1, chips):
        go(hop(step, col))
    go(pair(0, col))

    frame = jnp.zeros((PAD, LANES), jnp.float32)
    for c in range(chunks):
        beam[edge + c, pl.ds(0, PAD), :] = frame
        beam[edge + c, pl.ds(PAD + side, PAD), :] = frame

    def blank(step, _):
        at = pl.multiple_of(step * PAD, PAD)
        for c in list(range(edge)) + list(range(edge + chunks, 2 * edge + chunks)):
            beam[c, pl.ds(at, PAD), :] = frame
        return 0

    lax.fori_loop(0, side // PAD + 2, blank, 0)

    def gap(entry, _):
        at = pl.multiple_of(entry * (side + PAD), PAD)
        for q in range(parts):
            rolled[q][0, pl.ds(at, PAD), :] = frame
        return 0

    lax.fori_loop(0, FRONT + 1, gap, 0)
    image[parts, pl.ds(0, 8), :] = jnp.zeros((8, LANES), jnp.float32)
    make_lists(row, col, tile_rows, tile_cols, side, pixel_ref, lists, front)
    front_copy = pltpu.make_async_copy(front, front_list, front_sem)
    front_copy.start()

    def pick(position, carry):
        lane = lax.broadcasted_iota(jnp.int32, (8, LANES), 1)
        code = code_ref[len(rows_done) * total + position]
        which = position & (LANES - 1)
        line = image[code >> CHUNK_BIT, pl.ds((code >> LINE_BIT) & LINE_MASK, 1), :]
        moved = pltpu.roll(jnp.broadcast_to(line, (8, LANES)), code & (LANES - 1), 1)
        return jnp.where(lane == which, moved, carry)

    for copy in image_loads:
        copy.wait()
    zero = jnp.zeros((8, LANES), jnp.float32)
    sublane = lax.broadcasted_iota(jnp.int32, (8, LANES), 0)
    picked = []
    for g in range(groups):
        found = lax.fori_loop(g * LANES, (g + 1) * LANES, pick, zero, unroll=32)
        picked.append(jnp.where(sublane == len(rows_done), found, 0.0))
    front_copy.wait()

    band = side // 8
    unit = band // PIECES

    def roll_piece(piece):
        def several(step, _):
            for u in range(GROUP):
                entry = step * GROUP + u
                chunk, shift = front_list[0, entry], front_list[1, entry]
                turn = (LANES - shift) & (LANES - 1)
                keep = lane_iota(unit) >= shift
                for b in range(8):
                    at = b * band + piece * unit
                    cells = [beam[chunk + q, pl.ds(PAD + at, unit), :] for q in range(parts + 1)]
                    goal = pl.multiple_of(entry * (side + PAD) + PAD + at, 8)
                    for q in range(parts):
                        window = jnp.where(keep, cells[q], cells[q + 1])
                        rolled[q][0, pl.ds(goal, unit), :] = pltpu.roll(window, turn, 1)
            return 0

        lax.fori_loop(0, FRONT // GROUP, several, 0)

    for step in range(1, chips):
        source = lax.rem(col - 2 * step + n_col, n_col)
        hop(step, source).wait_recv()
        go(pair(step, source))
    for step in range(chips):
        source = lax.rem(partner[1] - 2 * step + n_col, n_col)
        pair(step, source).wait_recv()

    for g in range(groups):
        active = [(t, need) for t, need in enumerate(rows_done) if need > g * LANES]
        bounds = sorted({min(need, (g + 1) * LANES) for _, need in active})
        carry = zero
        start = g * LANES
        for stop in bounds:
            live = [t for t, need in active if min(need, (g + 1) * LANES) >= stop]

            def look(position, acc):
                lane = lax.broadcasted_iota(jnp.int32, (8, LANES), 1)
                here = lane == (position & (LANES - 1))
                for t in live:
                    code = code_ref[t * total + position]
                    line = beam[code >> CHUNK_BIT, pl.ds((code >> LINE_BIT) & LINE_MASK, 1), :]
                    moved = pltpu.roll(jnp.broadcast_to(line, (8, LANES)), code & (LANES - 1), 1)
                    acc = jnp.where(here & (sublane == t), moved, acc)
                return acc

            carry = lax.fori_loop(start, stop, look, carry, unroll=16)
            start = stop
        table[me, pl.ds(g * 8, 8), :] = carry + picked[g]

    def small(offset, target, slot):
        return pltpu.make_async_remote_copy(
            src_ref=table.at[slot],
            dst_ref=table.at[slot],
            send_sem=small_send.at[offset],
            recv_sem=small_recv.at[offset],
            device_id=(target // n_col, lax.rem(target, n_col)),
            device_id_type=MESH,
        )

    def spread(offset, _):
        small(offset, lax.rem(me + offset, n_dev), me).start()
        return 0

    lax.fori_loop(1, n_dev, spread, 0)

    def every(piece, _):
        roll_piece(piece)
        return 0

    lax.fori_loop(0, PIECES, every, 0)
    for copy in started:
        copy.wait_send()

    def collect(offset, _):
        other = lax.rem(me - offset + n_dev, n_dev)
        small(offset, other, other).wait_recv()
        small(offset, other, me).wait_send()
        return 0

    lax.fori_loop(1, n_dev, collect, 0)

    values = []
    for g in range(groups):
        part = table[:, g * 8 + len(rows_done), :]
        values.append(jnp.sum(part, axis=0, keepdims=True))
    lane = lax.broadcasted_iota(jnp.int32, (1, LANES), 1)
    amps = [jnp.zeros((1, LANES), jnp.float32) for _ in range(groups)]
    piece = min(n_dev, peaks)
    for r in range(rounds):
        g_here = r * peaks // LANES
        lane_here = r * peaks % LANES
        taken = jnp.zeros((1, LANES), jnp.float32)
        if r:
            for first in range(r * peaks, (r + 1) * peaks, piece):
                device, slot = first % n_dev, first // n_dev - skip
                dots = jnp.zeros((piece, LANES), jnp.float32)
                for g in range((r * peaks + LANES - 1) // LANES):
                    rows = table[device : device + piece, g * 8 + slot, :]
                    dots = dots + rows * amps[g]
                sums = jnp.sum(dots, axis=1, keepdims=True)
                spot = lax.broadcasted_iota(jnp.int32, (piece, LANES), 0) + first % LANES
                diag = spot == lax.broadcasted_iota(jnp.int32, (piece, LANES), 1)
                taken = taken + jnp.sum(jnp.where(diag, sums, 0.0), axis=0, keepdims=True)
        fresh = loop_gain * (values[g_here] - taken)
        mine = (lane >= lane_here) & (lane < lane_here + peaks)
        amps[g_here] = jnp.where(mine, fresh, amps[g_here])

    for g in range(groups):
        amp_out[0:1, g * LANES : (g + 1) * LANES] = amps[g]


def relay_kernel(
    n_row, n_col, rounds, peaks,
    pixel_ref, psf_ref, res_ref,
    beam, lists, amp_out, *rest,
):
    parts = res_ref.shape[1] // LANES
    rolled = rest[:parts]
    stage = rest[parts : parts + PIECES]
    (
        image, quarter, front, front_list, code_line, code_list, down, plane, table,
        load_sem, image_sem, front_sem, code_sem, send_sem, recv_sem, pair_send, pair_recv,
        plane_send, plane_recv, line_send, line_recv,
    ) = rest[parts + PIECES :]
    side = psf_ref.shape[1]
    chunks = side // LANES
    edge = parts
    depth = side // n_col
    total = rounds * peaks
    groups = total // LANES
    tile_rows, tile_cols = res_ref.shape
    strip = depth // PIECES
    row = lax.axis_index("row")
    col = lax.axis_index("col")
    core = lax.rem(col, 2)
    base = col - core
    flip = lax.rem(row, 2)
    near = col + 2 - 4 * lax.rem(col // 2, 2)
    far = col + 4 - 8 * (col // 4)
    across = near + far - col
    first = near + flip * (far - near)
    second = far + flip * (near - far)
    partner = (row, base + 1 - core)
    layer = (row + 1 - 2 * flip, col)
    place = row * 2 + core
    spots = 2 * n_row

    def lined(other):
        return (other // 2, base + lax.rem(other, 2))

    own_loads = [
        pltpu.make_async_copy(
            psf_ref.at[:, pl.ds(c * LANES, LANES)],
            quarter.at[edge + c, pl.ds(8 + core * depth, depth), :],
            load_sem.at[c],
        )
        for c in range(chunks)
    ]
    for copy in own_loads:
        copy.start()
    image_loads = [
        pltpu.make_async_copy(
            res_ref.at[:, pl.ds(u * LANES, LANES)],
            image.at[pl.ds(u * tile_rows, tile_rows), :],
            image_sem.at[u],
        )
        for u in range(parts)
    ]
    for copy in image_loads:
        copy.start()

    barrier = pltpu.get_barrier_semaphore()
    for device in [(row, near), (row, far), (row, across)] + [
        lined(lax.rem(place + offset, spots)) for offset in range(1, spots)
    ]:
        pl.semaphore_signal(barrier, inc=1, device_id=device, device_id_type=MESH)

    rim = list(range(edge)) + list(range(edge + chunks, 2 * edge + chunks))
    for c in range(2 * edge + chunks):
        quarter[c, 0:8, :] = jnp.zeros((8, LANES), jnp.float32)
    for c in rim:
        quarter[c, 8:, :] = jnp.zeros((2 * depth, LANES), jnp.float32)
        for p in range(PIECES):
            stage[p][c, :, :] = jnp.zeros((6 * strip, LANES), jnp.float32)
    image[pl.ds(parts * tile_rows, 8), :] = jnp.zeros((8, LANES), jnp.float32)

    lane = lane_iota(1)
    for axis in range(2):
        line = to_sublanes(pixel_ref[axis : axis + 1, :].astype(jnp.float32))
        down[axis, :, :] = jnp.broadcast_to(line.astype(jnp.int32), (total, LANES))
    for r in range(1, rounds):
        goal_row = down[0, pl.ds(r * peaks + place * 8, 8), :]
        goal_col = down[1, pl.ds(r * peaks + place * 8, 8), :]
        for g in range((r * peaks + LANES - 1) // LANES):
            cut = slice(g * LANES, (g + 1) * LANES)
            di = goal_row - pixel_ref[0:1, cut] + (side // 2 - base * depth)
            dj = goal_col - pixel_ref[1:2, cut] + side // 2
            valid = (di >= 0) & (di < 2 * depth) & (dj >= 0) & (dj < side)
            valid = valid & (lane + g * LANES < r * peaks)
            code = ((dj >> LINE_BIT) + edge << CHUNK_BIT) + (di + 8 << LINE_BIT)
            code = code + ((lane - dj) & (LANES - 1))
            at = ((r - 1) * groups + g) * 8
            code_line[at : at + 8, :] = jnp.where(valid, code, 0)
    tail = (rounds - 1) * groups * 8
    for g in range(groups):
        cut = slice(g * LANES, (g + 1) * LANES)
        lr = pixel_ref[0:1, cut] - row * tile_rows
        lc = pixel_ref[1:2, cut] - col * tile_cols
        own = (lr >= 0) & (lr < tile_rows) & (lc >= 0) & (lc < tile_cols)
        flat = jnp.where(own, (lc >> LINE_BIT) * tile_rows + lr, parts * tile_rows)
        code = (flat << LINE_BIT) + ((lane - lc) & (LANES - 1))
        code_line[tail + g : tail + g + 1, :] = code
    code_copy = pltpu.make_async_copy(code_line, code_list, code_sem)
    code_copy.start()

    for copy in own_loads:
        copy.wait()
    pl.semaphore_wait(barrier, 3 + spots - 1)

    started = []

    def remote(src, dst, device, send, recv):
        return pltpu.make_async_remote_copy(
            src_ref=src, dst_ref=dst, send_sem=send, recv_sem=recv,
            device_id=device, device_id_type=MESH,
        )

    def go(copy):
        copy.start()
        started.append(copy)

    def slot(p, kind, side_of):
        return stage[p].at[pl.ds(edge, chunks), pl.ds((kind * 2 + side_of) * strip, strip), :]

    def mine(p):
        return quarter.at[pl.ds(edge, chunks), pl.ds(8 + core * depth + p * strip, strip), :]

    def direct(p):
        return remote(
            mine(p), slot(p, 0, core), (row, first), send_sem.at[0, p], recv_sem.at[0, p]
        )

    def relay(p):
        return remote(
            slot(p, 0, core), slot(p, 1, core), (row, second), send_sem.at[1, p], recv_sem.at[1, p]
        )

    def lift(p):
        return remote(
            slot(p, 0, core), slot(p, 2, core), layer, send_sem.at[2, p], recv_sem.at[2, p]
        )

    def pair(kind, p, side_of):
        at = slot(p, kind, side_of)
        return remote(at, at, partner, pair_send.at[kind, p], pair_recv.at[kind, p])

    def pair_own(side_of):
        at = quarter.at[pl.ds(edge, chunks), pl.ds(8 + side_of * depth, depth), :]
        return remote(at, at, partner, pair_send.at[3, 0], pair_recv.at[3, 0])

    go(pair_own(core))
    for p in range(PIECES):
        go(direct(p))

    make_lists(row, col, tile_rows, tile_cols, side, pixel_ref, lists, front)
    front_copy = pltpu.make_async_copy(front, front_list, front_sem)
    front_copy.start()
    code_copy.wait()
    for copy in image_loads:
        copy.wait()
    sublane = lax.broadcasted_iota(jnp.int32, (8, LANES), 0)
    across_lane = lane_iota(8)

    def fetch(line, code):
        return pltpu.roll(jnp.broadcast_to(line, (8, LANES)), code & (LANES - 1), 1)

    picked = jnp.zeros((8, LANES), jnp.float32)
    for g in range(groups):

        def pick(at, carry):
            hit = (across_lane == at) & (sublane == g)
            code = code_list[tail + g, at]
            return jnp.where(hit, fetch(image[pl.ds(code >> LINE_BIT, 1), :], code), carry)

        picked = lax.fori_loop(0, LANES, pick, picked, unroll=32)

    wells = [(r, g) for r in range(1, rounds) for g in range((r * peaks + LANES - 1) // LANES)]

    def look(begin, end, found):
        g = begin // LANES
        live = [w for w, (r, h) in enumerate(wells) if h == g and r * peaks > begin]

        def one(at, held):
            held = list(held)
            here = across_lane == at
            for i in range(8):
                hit = here & (sublane == i)
                for w in live:
                    spot = ((wells[w][0] - 1) * groups + g) * 8 + i
                    code = code_list[spot, at]
                    line = quarter[code >> CHUNK_BIT, pl.ds((code >> LINE_BIT) & LINE_MASK, 1), :]
                    held[w] = jnp.where(hit, fetch(line, code), held[w])
            return tuple(held)

        return lax.fori_loop(begin - g * LANES, end - g * LANES, one, found, unroll=2)

    rows_of = [
        (None, 0, base * depth), (None, 1, (base + 1) * depth),
    ] + [
        (kind, other, (block - core + other) * depth)
        for kind, block in enumerate((first, across, second))
        for other in range(2)
    ]

    def cell(piece, kind, other, chunk):
        if kind is None:
            return quarter[chunk, pl.ds(8 + other * depth + piece * strip, strip), :]
        return stage[piece][chunk, pl.ds((kind * 2 + other) * strip, strip), :]

    def roll_piece(piece):
        for kind, other, start in rows_of:
            at = pl.multiple_of(PAD + start + piece * strip, 8)
            for c in range(chunks):
                beam[edge + c, pl.ds(at, strip), :] = cell(piece, kind, other, edge + c)

        def several(step, _):
            for u in range(GROUP):
                entry = step * GROUP + u
                chunk, shift = front_list[0, entry], front_list[1, entry]
                turn = (LANES - shift) & (LANES - 1)
                keep = lane_iota(strip) >= shift
                for kind, other, start in rows_of:
                    cells = [cell(piece, kind, other, chunk + q) for q in range(parts + 1)]
                    goal = entry * (side + PAD) + PAD + start + piece * strip
                    goal = pl.multiple_of(goal, 8)
                    for q in range(parts):
                        window = jnp.where(keep, cells[q], cells[q + 1])
                        rolled[q][0, pl.ds(goal, strip), :] = pltpu.roll(window, turn, 1)
            return 0

        lax.fori_loop(0, FRONT // GROUP, several, 0)

    def swap(j):
        device = (row, (near, far, across)[j])
        return remote(
            plane.at[0], plane.at[1 + j], device, plane_send.at[j], plane_recv.at[j]
        )

    def spread(offset, owner):
        return remote(
            table.at[owner], table.at[owner], lined(lax.rem(place + offset, spots)),
            line_send.at[offset], line_recv.at[offset],
        )

    looks = [
        [(0, peaks // 2)], [(peaks // 2, peaks)], [(peaks, 2 * peaks - peaks // 4)],
        [(2 * peaks - peaks // 4, 2 * peaks), (2 * peaks, 3 * peaks)],
    ]
    found = tuple(jnp.zeros((8, LANES), jnp.float32) for _ in wells)
    frame = jnp.zeros((PAD, LANES), jnp.float32)
    pair_own(1 - core).wait_recv()
    for p in range(PIECES + LAG):
        if p < PIECES:
            direct(p).wait_recv()
            go(relay(p))
            go(lift(p))
            go(pair(0, p, core))
        if p >= LAG:
            q = p - LAG
            relay(q).wait_recv()
            go(pair(1, q, core))
            lift(q).wait_recv()
            go(pair(2, q, core))
        if p < len(looks):
            for begin, end in looks[p]:
                found = look(begin, end, found)
        if p == len(looks) - 1:
            for w, part in enumerate(found):
                plane[0, w * 8 : w * 8 + 8, :] = part
            plane[0, len(wells) * 8 :, :] = picked
            for j in range(3):
                go(swap(j))
            for c in range(chunks):
                beam[edge + c, pl.ds(0, PAD), :] = frame
                beam[edge + c, pl.ds(PAD + side, PAD), :] = frame

            def blank(step, _):
                at = pl.multiple_of(step * PAD, PAD)
                for c in rim:
                    beam[c, pl.ds(at, PAD), :] = frame
                return 0

            lax.fori_loop(0, side // PAD + 2, blank, 0)

            def gap(entry, _):
                at = pl.multiple_of(entry * (side + PAD), PAD)
                for q in range(parts):
                    rolled[q][0, pl.ds(at, PAD), :] = frame
                return 0

            lax.fori_loop(0, FRONT + 1, gap, 0)
            front_copy.wait()
        if p > LAG:
            q = p - LAG - 1
            for kind in range(3):
                pair(kind, q, 1 - core).wait_recv()
            roll_piece(q)
        if p == len(looks) + 1:
            for j in range(3):
                swap(j).wait_recv()
            table[place, :, :] = plane[0] + plane[1] + plane[2] + plane[3]
            for offset in range(1, spots):
                go(spread(offset, place))
    for kind in range(3):
        pair(kind, PIECES - 1, 1 - core).wait_recv()
    roll_piece(PIECES - 1)
    for offset in range(1, spots):
        spread(offset, lax.rem(place - offset + spots, spots)).wait_recv()

    values = sum(table[z, len(wells) * 8 :, :] for z in range(spots))
    values = [values[g : g + 1, :] for g in range(groups)]
    amps = [jnp.zeros((1, LANES), jnp.float32) for _ in range(groups)]
    for r in range(rounds):
        g_here, lane_here = r * peaks // LANES, r * peaks % LANES
        taken = jnp.zeros((1, LANES), jnp.float32)
        if r:
            dots = jnp.zeros((peaks, LANES), jnp.float32)
            for w, (s, g) in enumerate(wells):
                if s == r:
                    rows = jnp.concatenate(
                        [table[z, w * 8 : w * 8 + 8, :] for z in range(spots)], axis=0
                    )
                    dots = dots + rows * amps[g]
            sums = jnp.sum(dots, axis=1, keepdims=True)
            spot = lax.broadcasted_iota(jnp.int32, (peaks, LANES), 0) + lane_here
            taken = jnp.sum(
                jnp.where(spot == lane_iota(peaks), sums, 0.0), axis=0, keepdims=True
            )
        fresh = loop_gain * (values[g_here] - taken)
        here = (lane >= lane_here) & (lane < lane_here + peaks)
        amps[g_here] = jnp.where(here, fresh, amps[g_here])
    for g in range(groups):
        amp_out[0:1, g * LANES : (g + 1) * LANES] = amps[g]
    for copy in started:
        copy.wait_send()


def subtract_kernel(
    rounds, peaks, side,
    lists_ref, res_ref, beam_ref, amps_ref, *rest,
):
    tile_rows, tile_cols = res_ref.shape
    pitch_rows = side + 2 * PAD
    parts = tile_cols // LANES
    blocks = tile_rows // PAD
    rolled = rest[:parts]
    (
        clean_ref, peak_ref, amp_ref,
        image, lists, amp_list, image_sem, store_sem, list_sem, amp_sem,
    ) = rest[parts:]

    copies = [
        pltpu.make_async_copy(lists_ref, lists, list_sem),
        pltpu.make_async_copy(amps_ref, amp_list, amp_sem),
    ]
    for copy in copies:
        copy.start()
    share = tile_rows // LOADS
    loads = [
        pltpu.make_async_copy(
            res_ref.at[pl.ds(i * share, share), :], image.at[pl.ds(i * share, share), :],
            image_sem.at[i],
        )
        for i in range(LOADS)
    ]
    for copy in loads:
        copy.start()
    for r in range(rounds):
        amp_ref[r : r + 1, :] = amps_ref[0:1, r * peaks : (r + 1) * peaks]
    for copy in copies:
        copy.wait()

    def store(block):
        at = pl.multiple_of(block * PAD, PAD)
        return pltpu.make_async_copy(
            image.at[pl.ds(at, PAD), :], clean_ref.at[pl.ds(at, PAD), :], store_sem.at[block]
        )

    lanes = lane_iota(PAD)

    def settle(block, best):
        at = pl.multiple_of(block * PAD, PAD)

        def ready(begin, step, held):
            held = list(held)
            for u in range(STRIDE):
                entry = begin + step * STRIDE + u
                first = lists[1, entry] + jnp.maximum(at - lists[0, entry], -PAD)
                amplitude = amp_list[0, lists[2, entry]]
                for q in range(parts):
                    held[q] = held[q] - amplitude * rolled[q][pl.ds(first, PAD), :]
            return tuple(held)

        def several(begin, step, held):
            held = list(held)
            for u in range(AHEAD):
                entry = begin + step * AHEAD + u
                first = lists[4, entry] + jnp.maximum(at - lists[3, entry], -PAD)
                amplitude = amp_list[0, lists[5, entry]]
                shift = lists[6, entry]
                turn = (LANES - shift) & (LANES - 1)
                keep = lanes >= shift
                cells = [
                    beam_ref[pl.ds(first + q * pitch_rows, PAD), :] for q in range(parts + 1)
                ]
                for q in range(parts):
                    moved = pltpu.roll(jnp.where(keep, cells[q], cells[q + 1]), turn, 1)
                    held[q] = held[q] - amplitude * moved
            return tuple(held)

        held = tuple(image[pl.ds(at, PAD), q * LANES : (q + 1) * LANES] for q in range(parts))
        for at_list, width, body in ((0, STRIDE, ready), (LANES, AHEAD, several)):
            begin, end = lists[7, at_list + blocks + block], lists[7, at_list + block]
            trips = (end - begin + width - 1) // width
            held = lax.fori_loop(0, trips, functools.partial(body, begin), held)
        for q in range(parts):
            image[pl.ds(at, PAD), q * LANES : (q + 1) * LANES] = held[q]
            for i in range(0, PAD, 8):
                best = jnp.maximum(best, jnp.abs(held[q][i : i + 8, :]))
        store(block).start()
        return best

    best = jnp.zeros((8, LANES), jnp.float32)
    for i in range(LOADS):
        loads[i].wait()
        best = lax.fori_loop(i * blocks // LOADS, (i + 1) * blocks // LOADS, settle, best)
    peak_ref[...] = jnp.max(jnp.max(best, axis=0, keepdims=True), axis=1, keepdims=True)

    def finish(block, _):
        store(block).wait()
        return 0

    lax.fori_loop(0, blocks, finish, 0)


def lookup_codes(n_row, n_col, tile_rows, tile_cols, side, peak_pixels):
    n_dev = n_row * n_col
    chunks = side // LANES
    half_width = side // 2
    rounds, peaks, _ = peak_pixels.shape
    total = rounds * peaks
    row_base = lax.axis_index("row") * tile_rows
    col_base = lax.axis_index("col") * tile_cols
    me = lax.axis_index("row") * n_col + lax.axis_index("col")
    parts = tile_cols // LANES

    per_device = total // n_dev
    skip = peaks // n_dev if peaks % n_dev == 0 else 0
    coeff_rows = per_device - skip
    if peaks % n_dev == 0:
        rows_done = tuple((t * n_dev // peaks) * peaks for t in range(skip, per_device))
    else:
        rows_done = (total,) * coeff_rows

    flat = peak_pixels.reshape(total, 2)
    prow, pcol = flat[:, 0], flat[:, 1]
    index = jnp.arange(total, dtype=jnp.int32)
    slots = lax.dynamic_slice(
        peak_pixels.reshape(per_device, n_dev, 2), (skip, me, 0), (coeff_rows, 1, 2)
    )
    target = me + n_dev * (jnp.arange(coeff_rows, dtype=jnp.int32) + skip)
    di = slots[:, :, 0] - prow[None, :] + half_width
    dj = slots[:, :, 1] - pcol[None, :] + half_width
    earlier = (index // peaks)[None, :] < (target // peaks)[:, None]
    valid = (di >= 0) & (di < side) & (dj >= 0) & (dj < side) & earlier
    look = (dj // LANES + parts << CHUNK_BIT) + (di + PAD << LINE_BIT)
    look = jnp.where(valid, look + (index[None, :] - dj) % LANES, 0)
    lr, lc = prow - row_base, pcol - col_base
    own = (lr >= 0) & (lr < tile_rows) & (lc >= 0) & (lc < tile_cols)
    pick = (lc // LANES << CHUNK_BIT) + (lr << LINE_BIT) + (index - lc) % LANES
    pick = jnp.where(own, pick, parts << CHUNK_BIT)
    codes = jnp.stack([*look, pick]).reshape(-1)
    return codes, skip, rows_done


def local(n_row, n_col, residual, point_spread, peak_pixels):
    n_dev = n_row * n_col
    tile_rows, tile_cols = residual.shape
    side = point_spread.shape[1]
    chunks = side // LANES
    rounds, peaks, _ = peak_pixels.shape
    total = rounds * peaks
    groups = total // LANES
    parts = tile_cols // LANES
    pixels = jnp.transpose(peak_pixels, (2, 0, 1)).reshape(2, total)

    smem = pl.BlockSpec(memory_space=pltpu.SMEM)
    vmem = pl.BlockSpec(memory_space=pltpu.VMEM)
    hbm = pl.BlockSpec(memory_space=pltpu.HBM)
    dma = pltpu.SemaphoreType.DMA
    padded = (chunks + 2 * parts, side + 2 * PAD, LANES)
    long = total + LANES
    reach = FRONT * (side + PAD) + PAD
    psf_hbm = pltpu.with_memory_space_constraint(point_spread, pltpu.HBM)
    res_hbm = pltpu.with_memory_space_constraint(residual, pltpu.HBM)
    results = (
        pltpu.VMEM(padded, jnp.float32),
        pltpu.VMEM((8, long), jnp.int32),
        pltpu.VMEM((1, total), jnp.float32),
        *[pltpu.VMEM((1, reach, LANES), jnp.float32)] * parts,
    )
    params = pltpu.CompilerParams(
        collective_id=0, has_side_effects=True, vmem_limit_bytes=SCRATCH
    )
    if (n_row, n_col) == (4, 8) and (rounds, peaks) == (4, 64):
        depth = side // n_col
        wells = sum((r * peaks + LANES - 1) // LANES for r in range(1, rounds))
        codes = (rounds - 1) * groups * 8 + 8
        beam, lists, amps, *rolled = pl.pallas_call(
            functools.partial(relay_kernel, n_row, n_col, rounds, peaks),
            out_shape=results,
            in_specs=[vmem, hbm, hbm],
            out_specs=(vmem,) * len(results),
            scratch_shapes=[
                *[pltpu.VMEM((padded[0], 6 * depth // PIECES, LANES), jnp.float32)] * PIECES,
                pltpu.VMEM((parts * tile_rows + 8, LANES), jnp.float32),
                pltpu.VMEM((padded[0], 8 + 2 * depth, LANES), jnp.float32),
                pltpu.VMEM((2, total), jnp.int32),
                pltpu.SMEM((2, total), jnp.int32),
                pltpu.VMEM((codes, LANES), jnp.int32),
                pltpu.SMEM((codes, LANES), jnp.int32),
                pltpu.VMEM((2, total, LANES), jnp.int32),
                pltpu.VMEM((4, wells * 8 + 8, LANES), jnp.float32),
                pltpu.VMEM((2 * n_row, wells * 8 + 8, LANES), jnp.float32),
                dma((chunks,)),
                dma((parts,)),
                dma,
                dma,
                dma((3, PIECES)),
                dma((3, PIECES)),
                dma((4, PIECES)),
                dma((4, PIECES)),
                dma((3,)),
                dma((3,)),
                dma((2 * n_row,)),
                dma((2 * n_row,)),
            ],
            compiler_params=params,
            name="gather_beam",
        )(pixels, psf_hbm, res_hbm)
    else:
        codes, skip, rows_done = lookup_codes(n_row, n_col, tile_rows, tile_cols, side, peak_pixels)
        beam, lists, amps, *rolled = pl.pallas_call(
            functools.partial(gather_kernel, n_row, n_col, skip, rows_done, rounds, peaks),
            out_shape=results,
            in_specs=[smem, vmem, hbm, hbm],
            out_specs=(vmem,) * len(results),
            scratch_shapes=[
                pltpu.VMEM((parts + 1, tile_rows, LANES), jnp.float32),
                pltpu.VMEM((2, total), jnp.int32),
                pltpu.SMEM((2, total), jnp.int32),
                pltpu.VMEM((n_dev, groups * 8, LANES), jnp.float32),
                dma((chunks,)),
                dma((parts,)),
                dma,
                dma((n_col,)),
                dma((n_col,)),
                dma((n_col,)),
                dma((n_col,)),
                dma((n_dev,)),
                dma((n_dev,)),
            ],
            compiler_params=params,
            name="gather_beam",
        )(codes, pixels, psf_hbm, res_hbm)

    cleaned, tile_peak, amps = pl.pallas_call(
        functools.partial(subtract_kernel, rounds, peaks, side),
        out_shape=(
            jax.ShapeDtypeStruct((tile_rows, tile_cols), jnp.float32),
            jax.ShapeDtypeStruct((1, 1), jnp.float32),
            jax.ShapeDtypeStruct((rounds, peaks), jnp.float32),
        ),
        in_specs=[vmem, hbm] + [vmem] * (2 + parts),
        out_specs=(hbm, vmem, vmem),
        scratch_shapes=[
            pltpu.VMEM((tile_rows, tile_cols), jnp.float32),
            pltpu.SMEM((8, long), jnp.int32),
            pltpu.SMEM((1, total), jnp.float32),
            dma((LOADS,)),
            dma((tile_rows // PAD,)),
            dma,
            dma,
        ],
        compiler_params=pltpu.CompilerParams(vmem_limit_bytes=4 << 20),
        name="subtract",
    )(
        lists,
        res_hbm,
        beam.reshape(padded[0] * padded[1], LANES),
        amps,
        *[part.reshape(reach, LANES) for part in rolled],
    )
    return cleaned, tile_peak, amps


def solution(mesh):
    return jax.shard_map(
        functools.partial(local, mesh.shape["row"], mesh.shape["col"]),
        mesh=mesh,
        in_specs=(P("row", "col"), P("col", None), P()),
        out_specs=(P("row", "col"), P("row", "col"), P()),
        check_vma=False,
    )
```

```python
import functools

import jax
import jax.numpy as jnp
from jax import lax
from jax.experimental import pallas as pl
from jax.experimental.pallas import tpu as pltpu
from jax.sharding import PartitionSpec as P

loop_gain = 0.1
LANES = 128
LINE_BIT = 7
CHUNK_BIT = 24
LINE_MASK = (1 << (CHUNK_BIT - LINE_BIT)) - 1
MESH = pl.DeviceIdType.MESH
PAD = 64
AHEAD = 8
STRIDE = 4
FRONT = 24
GROUP = 8
PIECES = 8
LAG = 2
QUEUED = 4
MEET = 4
SCRATCH = 11 << 20


def to_sublanes(line):
    square = lax.broadcasted_iota(jnp.int32, (LANES, LANES), 0) == lax.broadcasted_iota(
        jnp.int32, (LANES, LANES), 1
    )
    pieces = [
        jnp.sum(jnp.where(square, line[:, g : g + LANES], 0.0), axis=1, keepdims=True)
        for g in range(0, line.shape[1], LANES)
    ]
    return jnp.concatenate(pieces, axis=0)


def lane_iota(rows):
    return lax.broadcasted_iota(jnp.int32, (rows, LANES), 1)


def make_lists(row, col, tile_rows, tile_cols, side, pixels, lists, front):
    total = pixels.shape[1]
    spare = lists.shape[1] - total
    blocks = tile_rows // PAD
    pitch = side + 2 * PAD
    top = (pixels[0:1, :] - (row * tile_rows + side // 2)).astype(jnp.float32)
    left = (col * tile_cols + side // 2 - pixels[1:2, :]).astype(jnp.float32)
    inside = (top > -side) & (top < tile_rows) & (left > -tile_cols) & (left < side)
    start = jnp.clip(left.astype(jnp.int32) + tile_cols, 0, side + tile_cols - 1)
    height = jnp.minimum(top + side, tile_rows) - jnp.maximum(top, 0.0)
    height = jnp.where(inside, height, 0.0)
    index = lax.broadcasted_iota(jnp.int32, (1, total), 1).astype(jnp.float32)
    index_down = lax.broadcasted_iota(jnp.int32, (total, 1), 0).astype(jnp.float32)
    slot_at = lax.broadcasted_iota(jnp.int32, (total, total), 1).astype(jnp.float32)
    none, huge = -1.0, 1e9

    tall = index - height * total
    tall_down = to_sublanes(tall)
    rank_down = jnp.sum(jnp.where(tall < tall_down, 1.0, 0.0), axis=1, keepdims=True)
    rank = jnp.sum(jnp.where(tall_down < tall, 1.0, 0.0), axis=0, keepdims=True)
    in_down = to_sublanes(jnp.where(inside, 1.0, 0.0))
    chunk_down = to_sublanes((start >> LINE_BIT).astype(jnp.float32))
    shift_down = to_sublanes((start & (LANES - 1)).astype(jnp.float32))
    top_down = to_sublanes(top)

    def ordered(place_down, down, fill):
        picked = jnp.where(place_down == slot_at, down - fill, 0.0)
        return (jnp.sum(picked, axis=0, keepdims=True) + fill).astype(jnp.int32)

    last = (side + tile_cols - 1) >> LINE_BIT
    front[0:1, :] = jnp.clip(ordered(rank_down, chunk_down, 0.0), 0, last)
    front[1:2, :] = ordered(rank_down, shift_down, 0.0) & (LANES - 1)

    far = 4.0 * tile_rows
    by_top = top * total + index
    by_top_down = to_sublanes(by_top)
    bound = lane_iota(1)
    bound = jnp.where(bound < blocks, bound * PAD + PAD, (bound - blocks) * PAD - side + 1)
    bound = bound.astype(jnp.float32)
    line = 0
    for early in (True, False):
        chosen = inside & ((rank < FRONT) if early else (rank >= FRONT))
        side_down = (rank_down < FRONT) if early else (rank_down >= FRONT)
        chosen_down = jnp.where(side_down, in_down, 0.0)
        key = jnp.where(chosen, by_top, huge)
        place = jnp.sum(jnp.where(key < by_top_down, 1.0, 0.0), axis=1, keepdims=True)
        place = jnp.where(chosen_down > 0.0, place, none)
        if early:
            columns = [(top_down, far), (rank_down * (side + PAD) + PAD, PAD), (index_down, 0.0)]
        else:
            columns = [
                (top_down, far), (chunk_down * pitch + PAD, PAD),
                (index_down, 0.0), (shift_down, 0.0),
            ]
        for down, fill in columns:
            lists[line : line + 1, :total] = ordered(place, down, fill)
            lists[line : line + 1, total:] = jnp.full((1, spare), int(fill), jnp.int32)
            line += 1
        below = jnp.where(top_down < bound, chosen_down, 0.0)
        count = jnp.sum(below, axis=0, keepdims=True).astype(jnp.int32)
        at = 0 if early else LANES
        lists[7:8, at : at + LANES] = count


def gather_kernel(
    n_row, n_col, skip, rows_done, rounds, peaks,
    code_ref, pixel_ref, psf_ref, res_ref,
    beam, lists, amp_out, image, *rest,
):
    parts = res_ref.shape[1] // LANES
    rolled = rest[:parts]
    (
        front, front_list, table, load_sem, image_sem, front_sem,
        send_sem, recv_sem, pair_send, pair_recv, small_send, small_recv,
    ) = rest[parts:]
    n_dev = n_row * n_col
    side = psf_ref.shape[1]
    chunks = side // LANES
    edge = (beam.shape[0] - chunks) // 2
    depth = side // n_col
    total = rounds * peaks
    groups = total // LANES
    row = lax.axis_index("row")
    col = lax.axis_index("col")
    me = row * n_col + col
    tile_rows, tile_cols = res_ref.shape

    own_loads = [
        pltpu.make_async_copy(
            psf_ref.at[:, pl.ds(c * LANES, LANES)],
            beam.at[edge + c, pl.ds(PAD + col * depth, depth), :],
            load_sem.at[c],
        )
        for c in range(chunks)
    ]
    for copy in own_loads:
        copy.start()
    image_loads = [
        pltpu.make_async_copy(
            res_ref.at[:, pl.ds(u * LANES, LANES)],
            image.at[pl.ds(u * tile_rows, tile_rows), :],
            image_sem.at[u],
        )
        for u in range(parts)
    ]
    for copy in image_loads:
        copy.start()

    barrier = pltpu.get_barrier_semaphore()

    def greet(offset, _):
        other = lax.rem(me + offset, n_dev)
        pl.semaphore_signal(
            barrier, inc=1, device_id=(other // n_col, lax.rem(other, n_col)), device_id_type=MESH
        )
        return 0

    lax.fori_loop(1, n_dev, greet, 0)
    for copy in own_loads:
        copy.wait()
    pl.semaphore_wait(barrier, n_dev - 1)

    def remote(block, device, send, recv):
        region = beam.at[pl.ds(edge, chunks), pl.ds(PAD + block * depth, depth), :]
        return pltpu.make_async_remote_copy(
            src_ref=region,
            dst_ref=region,
            send_sem=send,
            recv_sem=recv,
            device_id=device,
            device_id_type=MESH,
        )

    started = []

    def go(copy):
        copy.start()
        started.append(copy)

    partner = (row, col + 1 - 2 * lax.rem(col, 2))
    chips = n_col // 2

    def hop(step, block):
        target = (row, lax.rem(col + 2 * step, n_col))
        return remote(block, target, send_sem.at[step], recv_sem.at[step])

    def pair(step, block):
        return remote(block, partner, pair_send.at[step], pair_recv.at[step])

    for step in range(1, chips):
        go(hop(step, col))
    go(pair(0, col))

    frame = jnp.zeros((PAD, LANES), jnp.float32)
    for c in range(chunks):
        beam[edge + c, pl.ds(0, PAD), :] = frame
        beam[edge + c, pl.ds(PAD + side, PAD), :] = frame

    def blank(step, _):
        at = pl.multiple_of(step * PAD, PAD)
        for c in list(range(edge)) + list(range(edge + chunks, 2 * edge + chunks)):
            beam[c, pl.ds(at, PAD), :] = frame
        return 0

    lax.fori_loop(0, side // PAD + 2, blank, 0)

    def gap(entry, _):
        at = pl.multiple_of(entry * (side + PAD), PAD)
        for q in range(parts):
            rolled[q][0, pl.ds(at, PAD), :] = frame
        return 0

    lax.fori_loop(0, FRONT + 1, gap, 0)
    image[pl.ds(parts * tile_rows, 8), :] = jnp.zeros((8, LANES), jnp.float32)
    make_lists(row, col, tile_rows, tile_cols, side, pixel_ref, lists, front)
    front_copy = pltpu.make_async_copy(front, front_list, front_sem)
    front_copy.start()

    def pick(position, carry):
        lane = lax.broadcasted_iota(jnp.int32, (8, LANES), 1)
        code = code_ref[len(rows_done) * total + position]
        which = position & (LANES - 1)
        line = image[pl.ds(code >> LINE_BIT, 1), :]
        moved = pltpu.roll(jnp.broadcast_to(line, (8, LANES)), code & (LANES - 1), 1)
        return jnp.where(lane == which, moved, carry)

    for copy in image_loads:
        copy.wait()
    zero = jnp.zeros((8, LANES), jnp.float32)
    sublane = lax.broadcasted_iota(jnp.int32, (8, LANES), 0)
    picked = []
    for g in range(groups):
        found = lax.fori_loop(g * LANES, (g + 1) * LANES, pick, zero, unroll=32)
        picked.append(jnp.where(sublane == len(rows_done), found, 0.0))
    front_copy.wait()

    band = side // 8
    unit = band // PIECES

    def roll_piece(piece):
        def several(step, _):
            for u in range(GROUP):
                entry = step * GROUP + u
                chunk, shift = front_list[0, entry], front_list[1, entry]
                turn = (LANES - shift) & (LANES - 1)
                keep = lane_iota(unit) >= shift
                for b in range(8):
                    at = b * band + piece * unit
                    cells = [beam[chunk + q, pl.ds(PAD + at, unit), :] for q in range(parts + 1)]
                    goal = pl.multiple_of(entry * (side + PAD) + PAD + at, 8)
                    for q in range(parts):
                        window = jnp.where(keep, cells[q], cells[q + 1])
                        rolled[q][0, pl.ds(goal, unit), :] = pltpu.roll(window, turn, 1)
            return 0

        lax.fori_loop(0, FRONT // GROUP, several, 0)

    for step in range(1, chips):
        source = lax.rem(col - 2 * step + n_col, n_col)
        hop(step, source).wait_recv()
        go(pair(step, source))
    for step in range(chips):
        source = lax.rem(partner[1] - 2 * step + n_col, n_col)
        pair(step, source).wait_recv()

    for g in range(groups):
        active = [(t, need) for t, need in enumerate(rows_done) if need > g * LANES]
        bounds = sorted({min(need, (g + 1) * LANES) for _, need in active})
        carry = zero
        start = g * LANES
        for stop in bounds:
            live = [t for t, need in active if min(need, (g + 1) * LANES) >= stop]

            def look(position, acc):
                lane = lax.broadcasted_iota(jnp.int32, (8, LANES), 1)
                here = lane == (position & (LANES - 1))
                for t in live:
                    code = code_ref[t * total + position]
                    line = beam[code >> CHUNK_BIT, pl.ds((code >> LINE_BIT) & LINE_MASK, 1), :]
                    moved = pltpu.roll(jnp.broadcast_to(line, (8, LANES)), code & (LANES - 1), 1)
                    acc = jnp.where(here & (sublane == t), moved, acc)
                return acc

            carry = lax.fori_loop(start, stop, look, carry, unroll=16)
            start = stop
        table[me, pl.ds(g * 8, 8), :] = carry + picked[g]

    def small(offset, target, slot):
        return pltpu.make_async_remote_copy(
            src_ref=table.at[slot],
            dst_ref=table.at[slot],
            send_sem=small_send.at[offset],
            recv_sem=small_recv.at[offset],
            device_id=(target // n_col, lax.rem(target, n_col)),
            device_id_type=MESH,
        )

    def spread(offset, _):
        small(offset, lax.rem(me + offset, n_dev), me).start()
        return 0

    lax.fori_loop(1, n_dev, spread, 0)

    def every(piece, _):
        roll_piece(piece)
        return 0

    lax.fori_loop(0, PIECES, every, 0)
    for copy in started:
        copy.wait_send()

    def collect(offset, _):
        other = lax.rem(me - offset + n_dev, n_dev)
        small(offset, other, other).wait_recv()
        small(offset, other, me).wait_send()
        return 0

    lax.fori_loop(1, n_dev, collect, 0)

    values = []
    for g in range(groups):
        part = table[:, g * 8 + len(rows_done), :]
        values.append(jnp.sum(part, axis=0, keepdims=True))
    lane = lax.broadcasted_iota(jnp.int32, (1, LANES), 1)
    amps = [jnp.zeros((1, LANES), jnp.float32) for _ in range(groups)]
    piece = min(n_dev, peaks)
    for r in range(rounds):
        g_here = r * peaks // LANES
        lane_here = r * peaks % LANES
        taken = jnp.zeros((1, LANES), jnp.float32)
        if r:
            for first in range(r * peaks, (r + 1) * peaks, piece):
                device, slot = first % n_dev, first // n_dev - skip
                dots = jnp.zeros((piece, LANES), jnp.float32)
                for g in range((r * peaks + LANES - 1) // LANES):
                    rows = table[device : device + piece, g * 8 + slot, :]
                    dots = dots + rows * amps[g]
                sums = jnp.sum(dots, axis=1, keepdims=True)
                spot = lax.broadcasted_iota(jnp.int32, (piece, LANES), 0) + first % LANES
                diag = spot == lax.broadcasted_iota(jnp.int32, (piece, LANES), 1)
                taken = taken + jnp.sum(jnp.where(diag, sums, 0.0), axis=0, keepdims=True)
        fresh = loop_gain * (values[g_here] - taken)
        mine = (lane >= lane_here) & (lane < lane_here + peaks)
        amps[g_here] = jnp.where(mine, fresh, amps[g_here])

    for g in range(groups):
        amp_out[0:1, g * LANES : (g + 1) * LANES] = amps[g]


def relay_kernel(
    n_row, n_col, rounds, peaks,
    pixel_ref, psf_ref, res_ref,
    beam, lists, amp_out, image, *rest,
):
    parts = res_ref.shape[1] // LANES
    rolled = rest[:parts]
    stage = rest[parts : parts + PIECES]
    (
        quarter, front, front_list, code_line, code_list, turns, down, plane, table,
        load_sem, image_sem, front_sem, code_sem, send_sem, recv_sem, pair_send, pair_recv,
        plane_send, plane_recv, line_send, line_recv,
    ) = rest[parts + PIECES :]
    side = psf_ref.shape[1]
    chunks = side // LANES
    edge = parts
    depth = side // n_col
    total = rounds * peaks
    groups = total // LANES
    tile_rows, tile_cols = res_ref.shape
    strip = depth // PIECES
    row = lax.axis_index("row")
    col = lax.axis_index("col")
    core = lax.rem(col, 2)
    base = col - core
    flip = lax.rem(row, 2)
    near = col + 2 - 4 * lax.rem(col // 2, 2)
    far = col + 4 - 8 * (col // 4)
    across = near + far - col
    first = near + flip * (far - near)
    second = far + flip * (near - far)
    partner = (row, base + 1 - core)
    layer = (row + 1 - 2 * flip, col)
    place = row * 2 + core
    spots = 2 * n_row

    def lined(other):
        return (other // 2, base + lax.rem(other, 2))

    own_loads = [
        pltpu.make_async_copy(
            psf_ref.at[:, pl.ds(c * LANES, LANES)],
            quarter.at[edge + c, pl.ds(8 + core * depth, depth), :],
            load_sem.at[c],
        )
        for c in range(chunks)
    ]
    for copy in own_loads:
        copy.start()
    image_loads = [
        pltpu.make_async_copy(
            res_ref.at[:, pl.ds(u * LANES, LANES)],
            image.at[pl.ds(u * tile_rows, tile_rows), :],
            image_sem.at[u],
        )
        for u in range(parts)
    ]
    for copy in image_loads:
        copy.start()

    barrier = pltpu.get_barrier_semaphore()
    for device in [(row, near), (row, far), (row, across)] + [
        lined(lax.rem(place + offset, spots)) for offset in range(1, spots)
    ]:
        pl.semaphore_signal(barrier, inc=1, device_id=device, device_id_type=MESH)

    rim = list(range(edge)) + list(range(edge + chunks, 2 * edge + chunks))
    for c in range(2 * edge + chunks):
        quarter[c, 0:8, :] = jnp.zeros((8, LANES), jnp.float32)
    for c in rim:
        quarter[c, 8:, :] = jnp.zeros((2 * depth, LANES), jnp.float32)
        for p in range(PIECES):
            stage[p][c, :, :] = jnp.zeros((6 * strip, LANES), jnp.float32)
    image[pl.ds(parts * tile_rows, 8), :] = jnp.zeros((8, LANES), jnp.float32)

    lane = lane_iota(1)
    sublane = lax.broadcasted_iota(jnp.int32, (8, LANES), 0)
    across_lane = lane_iota(8)
    spans, turned = [], []
    flat_rows = quarter.shape[1]
    for axis in range(2):
        line = to_sublanes(pixel_ref[axis : axis + 1, :].astype(jnp.float32))
        down[axis, :, :] = jnp.broadcast_to(line.astype(jnp.int32), (total, LANES))
    for r in range(1, rounds):
        goal_row = down[0, pl.ds(r * peaks + place * 8, 8), :]
        goal_col = down[1, pl.ds(r * peaks + place * 8, 8), :]
        for g in range((r * peaks + LANES - 1) // LANES):
            cut = slice(g * LANES, (g + 1) * LANES)
            di = goal_row - pixel_ref[0:1, cut] + (side // 2 - base * depth)
            dj = goal_col - pixel_ref[1:2, cut] + side // 2
            valid = (di >= 0) & (di < 2 * depth) & (dj >= 0) & (dj < side)
            valid = valid & (lane + g * LANES < r * peaks)
            code = ((dj >> LINE_BIT) + edge) * flat_rows + di + 8
            at = ((r - 1) * groups + g) * 8
            code_line[at : at + 8, :] = jnp.where(valid, code, 8) - sublane
            spans.append((r, g, len(turned), jnp.where(valid, dj & (LANES - 1), 0)))
            turned.extend(range(min(LANES, r * peaks - g * LANES)))
    tail = (rounds - 1) * groups * 8
    for g in range(groups):
        cut = slice(g * LANES, (g + 1) * LANES)
        lr = pixel_ref[0:1, cut] - row * tile_rows
        lc = pixel_ref[1:2, cut] - col * tile_cols
        own = (lr >= 0) & (lr < tile_rows) & (lc >= 0) & (lc < tile_cols)
        flat = jnp.where(own, (lc >> LINE_BIT) * tile_rows + lr, parts * tile_rows)
        code = (flat << LINE_BIT) + ((lane - lc) & (LANES - 1))
        code_line[tail + g : tail + g + 1, :] = code
    code_copy = pltpu.make_async_copy(code_line, code_list, code_sem)
    code_copy.start()

    for r, g, offset, column in spans:

        def splat(at, _):
            turns[offset + at, :, :] = jnp.take_along_axis(
                column, jnp.full((8, LANES), at, jnp.int32), axis=1
            )
            return 0

        lax.fori_loop(0, min(LANES, r * peaks - g * LANES), splat, 0, unroll=64)
    for copy in own_loads:
        copy.wait()
    pl.semaphore_wait(barrier, 3 + spots - 1)

    started = []

    def remote(src, dst, device, send, recv):
        return pltpu.make_async_remote_copy(
            src_ref=src, dst_ref=dst, send_sem=send, recv_sem=recv,
            device_id=device, device_id_type=MESH,
        )

    def go(copy):
        copy.start()
        started.append(copy)

    def slot(p, kind, side_of):
        return stage[p].at[pl.ds(edge, chunks), pl.ds((kind * 2 + side_of) * strip, strip), :]

    def mine(p):
        return quarter.at[pl.ds(edge, chunks), pl.ds(8 + core * depth + p * strip, strip), :]

    def direct(p):
        return remote(
            mine(p), slot(p, 0, core), (row, first), send_sem.at[0, p], recv_sem.at[0, p]
        )

    def relay(p):
        return remote(
            slot(p, 0, core), slot(p, 1, core), (row, second), send_sem.at[1, p], recv_sem.at[1, p]
        )

    def lift(p):
        return remote(
            slot(p, 0, core), slot(p, 2, core), layer, send_sem.at[2, p], recv_sem.at[2, p]
        )

    def pair(kind, p, side_of):
        at = slot(p, kind, side_of)
        return remote(at, at, partner, pair_send.at[kind, p], pair_recv.at[kind, p])

    def pair_own(side_of):
        at = quarter.at[pl.ds(edge, chunks), pl.ds(8 + side_of * depth, depth), :]
        return remote(at, at, partner, pair_send.at[3, 0], pair_recv.at[3, 0])

    go(pair_own(core))
    for p in range(QUEUED):
        go(direct(p))

    code_copy.wait()
    for copy in image_loads:
        copy.wait()

    def fetch(line, code):
        return pltpu.roll(jnp.broadcast_to(line, (8, LANES)), code & (LANES - 1), 1)

    picked = jnp.zeros((8, LANES), jnp.float32)
    for g in range(groups):

        def pick(at, carry):
            hit = (across_lane == at) & (sublane == g)
            code = code_list[tail + g, at]
            return jnp.where(hit, fetch(image[pl.ds(code >> LINE_BIT, 1), :], code), carry)

        picked = lax.fori_loop(0, LANES, pick, picked, unroll=32)

    wells = [(r, g, offset) for r, g, offset, _ in spans]
    flat_quarter = quarter.reshape((2 * edge + chunks) * flat_rows, LANES)

    def look(begin, end, found):
        g = begin // LANES
        live = [w for w, (r, h, _) in enumerate(wells) if h == g and r * peaks > begin]

        def one(at, held):
            held = list(held)
            here = across_lane == at
            for w in live:
                r, _, offset = wells[w]
                lines = jnp.zeros((8, LANES), jnp.float32)
                for i in range(8):
                    code = code_list[((r - 1) * groups + g) * 8 + i, at]
                    lines = jnp.where(sublane == i, flat_quarter[pl.ds(code, 8), :], lines)
                value = jnp.take_along_axis(lines, turns[offset + at, :, :], axis=1)
                held[w] = jnp.where(here, value, held[w])
            return tuple(held)

        return lax.fori_loop(begin - g * LANES, end - g * LANES, one, found, unroll=16)

    rows_of = [
        (None, 0, base * depth), (None, 1, (base + 1) * depth),
    ] + [
        (kind, other, (block - core + other) * depth)
        for kind, block in enumerate((first, across, second))
        for other in range(2)
    ]

    def cell(piece, kind, other, chunk):
        if kind is None:
            return quarter[chunk, pl.ds(8 + other * depth + piece * strip, strip), :]
        return stage[piece][chunk, pl.ds((kind * 2 + other) * strip, strip), :]

    def roll_piece(piece):
        for kind, other, start in rows_of:
            at = pl.multiple_of(PAD + start + piece * strip, 8)
            for c in range(chunks):
                beam[edge + c, pl.ds(at, strip), :] = cell(piece, kind, other, edge + c)

        def several(step, _):
            for u in range(GROUP):
                entry = step * GROUP + u
                chunk, shift = front_list[0, entry], front_list[1, entry]
                turn = (LANES - shift) & (LANES - 1)
                keep = lane_iota(strip) >= shift
                for kind, other, start in rows_of:
                    cells = [cell(piece, kind, other, chunk + q) for q in range(parts + 1)]
                    goal = entry * (side + PAD) + PAD + start + piece * strip
                    goal = pl.multiple_of(goal, 8)
                    for q in range(parts):
                        window = jnp.where(keep, cells[q], cells[q + 1])
                        rolled[q][0, pl.ds(goal, strip), :] = pltpu.roll(window, turn, 1)
            return 0

        lax.fori_loop(0, FRONT // GROUP, several, 0)

    def swap(j):
        device = (row, (near, far, across)[j])
        return remote(
            plane.at[0], plane.at[1 + j], device, plane_send.at[j], plane_recv.at[j]
        )

    def spread(offset, owner):
        return remote(
            table.at[owner], table.at[owner], lined(lax.rem(place + offset, spots)),
            line_send.at[offset], line_recv.at[offset],
        )

    found = tuple(jnp.zeros((8, LANES), jnp.float32) for _ in wells)
    frame = jnp.zeros((PAD, LANES), jnp.float32)
    pair_own(1 - core).wait_recv()
    for begin in range(0, (rounds - 1) * peaks, peaks):
        found = look(begin, begin + peaks, found)
    for w, part in enumerate(found):
        plane[0, w * 8 : w * 8 + 8, :] = part
    plane[0, len(wells) * 8 :, :] = picked
    for j in range(3):
        go(swap(j))
    for p in range(PIECES + LAG):
        if p < PIECES:
            direct(p).wait_recv()
            if p + QUEUED < PIECES:
                go(direct(p + QUEUED))
            go(relay(p))
            go(lift(p))
            go(pair(0, p, core))
        if p >= LAG:
            q = p - LAG
            relay(q).wait_recv()
            go(pair(1, q, core))
            lift(q).wait_recv()
            go(pair(2, q, core))
        if p == 0:
            make_lists(row, col, tile_rows, tile_cols, side, pixel_ref, lists, front)
            front_copy = pltpu.make_async_copy(front, front_list, front_sem)
            front_copy.start()
        if p == 1:
            for c in range(chunks):
                beam[edge + c, pl.ds(0, PAD), :] = frame
                beam[edge + c, pl.ds(PAD + side, PAD), :] = frame

            def blank(step, _):
                at = pl.multiple_of(step * PAD, PAD)
                for c in rim:
                    beam[c, pl.ds(at, PAD), :] = frame
                return 0

            lax.fori_loop(0, side // PAD + 2, blank, 0)

            def gap(entry, _):
                at = pl.multiple_of(entry * (side + PAD), PAD)
                for q in range(parts):
                    rolled[q][0, pl.ds(at, PAD), :] = frame
                return 0

            lax.fori_loop(0, FRONT + 1, gap, 0)
            front_copy.wait()
        if p == MEET:
            for j in range(3):
                swap(j).wait_recv()
            table[place, :, :] = plane[0] + plane[1] + plane[2] + plane[3]
            for offset in range(1, spots):
                go(spread(offset, place))
        if p > LAG:
            q = p - LAG - 1
            for kind in range(3):
                pair(kind, q, 1 - core).wait_recv()
            roll_piece(q)
    for kind in range(3):
        pair(kind, PIECES - 1, 1 - core).wait_recv()
    roll_piece(PIECES - 1)
    for offset in range(1, spots):
        spread(offset, lax.rem(place - offset + spots, spots)).wait_recv()

    values = sum(table[z, len(wells) * 8 :, :] for z in range(spots))
    values = [values[g : g + 1, :] for g in range(groups)]
    amps = [jnp.zeros((1, LANES), jnp.float32) for _ in range(groups)]
    for r in range(rounds):
        g_here, lane_here = r * peaks // LANES, r * peaks % LANES
        taken = jnp.zeros((1, LANES), jnp.float32)
        if r:
            dots = jnp.zeros((peaks, LANES), jnp.float32)
            for w, (s, g, _) in enumerate(wells):
                if s == r:
                    rows = jnp.concatenate(
                        [table[z, w * 8 : w * 8 + 8, :] for z in range(spots)], axis=0
                    )
                    dots = dots + rows * amps[g]
            sums = jnp.sum(dots, axis=1, keepdims=True)
            spot = lax.broadcasted_iota(jnp.int32, (peaks, LANES), 0) + lane_here
            taken = jnp.sum(
                jnp.where(spot == lane_iota(peaks), sums, 0.0), axis=0, keepdims=True
            )
        fresh = loop_gain * (values[g_here] - taken)
        here = (lane >= lane_here) & (lane < lane_here + peaks)
        amps[g_here] = jnp.where(here, fresh, amps[g_here])
    for g in range(groups):
        amp_out[0:1, g * LANES : (g + 1) * LANES] = amps[g]
    for copy in started:
        copy.wait_send()


def subtract_kernel(
    rounds, peaks, side,
    tile_rows, tile_cols, lists_ref, image_ref, beam_ref, amps_ref, *rest,
):
    pitch_rows = side + 2 * PAD
    parts = tile_cols // LANES
    blocks = tile_rows // PAD
    rolled = rest[:parts]
    (
        clean_ref, peak_ref, amp_ref,
        image, lists, amp_list, store_sem, list_sem, amp_sem,
    ) = rest[parts:]

    copies = [
        pltpu.make_async_copy(lists_ref, lists, list_sem),
        pltpu.make_async_copy(amps_ref, amp_list, amp_sem),
    ]
    for copy in copies:
        copy.start()
    for r in range(rounds):
        amp_ref[r : r + 1, :] = amps_ref[0:1, r * peaks : (r + 1) * peaks]
    for copy in copies:
        copy.wait()

    def store(block):
        at = pl.multiple_of(block * PAD, PAD)
        return pltpu.make_async_copy(
            image.at[pl.ds(at, PAD), :], clean_ref.at[pl.ds(at, PAD), :], store_sem.at[block]
        )

    lanes = lane_iota(PAD)

    def settle(block, best):
        at = pl.multiple_of(block * PAD, PAD)

        ready, ready_end = lists[7, blocks + block], lists[7, block]
        later, later_end = lists[7, LANES + blocks + block], lists[7, LANES + block]

        def still(entry, held):
            first = lists[1, entry] + jnp.maximum(at - lists[0, entry], -PAD)
            amplitude = amp_list[0, lists[2, entry]]
            return [
                held[q] - amplitude * rolled[q][pl.ds(first, PAD), :] for q in range(parts)
            ]

        def turning(entry, held):
            first = lists[4, entry] + jnp.maximum(at - lists[3, entry], -PAD)
            amplitude = amp_list[0, lists[5, entry]]
            shift = lists[6, entry]
            turn = (LANES - shift) & (LANES - 1)
            keep = lanes >= shift
            cells = [beam_ref[pl.ds(first + q * pitch_rows, PAD), :] for q in range(parts + 1)]
            moved = [
                pltpu.roll(jnp.where(keep, cells[q], cells[q + 1]), turn, 1) for q in range(parts)
            ]
            return [held[q] - amplitude * moved[q] for q in range(parts)]

        def both(step, held):
            held = list(held)
            for u in range(AHEAD):
                held = still(ready + step * AHEAD + u, held)
            for u in range(AHEAD):
                held = turning(later + step * AHEAD + u, held)
            return tuple(held)

        def rest_of(step, held):
            held = list(held)
            for u in range(STRIDE):
                held = still(ready + step * STRIDE + u, held)
            return tuple(held)

        held = tuple(image_ref[pl.ds(q * tile_rows + at, PAD), :] for q in range(parts))
        trips = (later_end - later + AHEAD - 1) // AHEAD
        held = lax.fori_loop(0, trips, both, held)
        more = (ready_end - ready + STRIDE - 1) // STRIDE
        held = lax.fori_loop(trips * (AHEAD // STRIDE), more, rest_of, held)
        for q in range(parts):
            image[pl.ds(at, PAD), q * LANES : (q + 1) * LANES] = held[q]
            for i in range(0, PAD, 8):
                best = jnp.maximum(best, jnp.abs(held[q][i : i + 8, :]))
        store(block).start()
        return best

    best = jnp.zeros((8, LANES), jnp.float32)
    best = lax.fori_loop(0, blocks, settle, best)
    peak_ref[...] = jnp.max(jnp.max(best, axis=0, keepdims=True), axis=1, keepdims=True)

    def finish(block, _):
        store(block).wait()
        return 0

    lax.fori_loop(0, blocks, finish, 0)


def lookup_codes(n_row, n_col, tile_rows, tile_cols, side, peak_pixels):
    n_dev = n_row * n_col
    chunks = side // LANES
    half_width = side // 2
    rounds, peaks, _ = peak_pixels.shape
    total = rounds * peaks
    row_base = lax.axis_index("row") * tile_rows
    col_base = lax.axis_index("col") * tile_cols
    me = lax.axis_index("row") * n_col + lax.axis_index("col")
    parts = tile_cols // LANES

    per_device = total // n_dev
    skip = peaks // n_dev if peaks % n_dev == 0 else 0
    coeff_rows = per_device - skip
    if peaks % n_dev == 0:
        rows_done = tuple((t * n_dev // peaks) * peaks for t in range(skip, per_device))
    else:
        rows_done = (total,) * coeff_rows

    flat = peak_pixels.reshape(total, 2)
    prow, pcol = flat[:, 0], flat[:, 1]
    index = jnp.arange(total, dtype=jnp.int32)
    slots = lax.dynamic_slice(
        peak_pixels.reshape(per_device, n_dev, 2), (skip, me, 0), (coeff_rows, 1, 2)
    )
    target = me + n_dev * (jnp.arange(coeff_rows, dtype=jnp.int32) + skip)
    di = slots[:, :, 0] - prow[None, :] + half_width
    dj = slots[:, :, 1] - pcol[None, :] + half_width
    earlier = (index // peaks)[None, :] < (target // peaks)[:, None]
    valid = (di >= 0) & (di < side) & (dj >= 0) & (dj < side) & earlier
    look = (dj // LANES + parts << CHUNK_BIT) + (di + PAD << LINE_BIT)
    look = jnp.where(valid, look + (index[None, :] - dj) % LANES, 0)
    lr, lc = prow - row_base, pcol - col_base
    own = (lr >= 0) & (lr < tile_rows) & (lc >= 0) & (lc < tile_cols)
    pick = (lc // LANES * tile_rows + lr << LINE_BIT) + (index - lc) % LANES
    pick = jnp.where(own, pick, parts * tile_rows << LINE_BIT)
    codes = jnp.stack([*look, pick]).reshape(-1)
    return codes, skip, rows_done


def local(n_row, n_col, residual, point_spread, peak_pixels):
    n_dev = n_row * n_col
    tile_rows, tile_cols = residual.shape
    side = point_spread.shape[1]
    chunks = side // LANES
    rounds, peaks, _ = peak_pixels.shape
    total = rounds * peaks
    groups = total // LANES
    parts = tile_cols // LANES
    pixels = jnp.transpose(peak_pixels, (2, 0, 1)).reshape(2, total)

    smem = pl.BlockSpec(memory_space=pltpu.SMEM)
    vmem = pl.BlockSpec(memory_space=pltpu.VMEM)
    hbm = pl.BlockSpec(memory_space=pltpu.HBM)
    dma = pltpu.SemaphoreType.DMA
    padded = (chunks + 2 * parts, side + 2 * PAD, LANES)
    long = total + LANES
    reach = FRONT * (side + PAD) + PAD
    psf_hbm = pltpu.with_memory_space_constraint(point_spread, pltpu.HBM)
    res_hbm = pltpu.with_memory_space_constraint(residual, pltpu.HBM)
    results = (
        pltpu.VMEM(padded, jnp.float32),
        pltpu.VMEM((8, long), jnp.int32),
        pltpu.VMEM((1, total), jnp.float32),
        pltpu.VMEM((parts * tile_rows + 8, LANES), jnp.float32),
        *[pltpu.VMEM((1, reach, LANES), jnp.float32)] * parts,
    )
    params = pltpu.CompilerParams(
        collective_id=0, has_side_effects=True, vmem_limit_bytes=SCRATCH
    )
    if (n_row, n_col) == (4, 8) and (rounds, peaks) == (4, 64):
        depth = side // n_col
        wells = sum((r * peaks + LANES - 1) // LANES for r in range(1, rounds))
        codes = (rounds - 1) * groups * 8 + 8
        beam, lists, amps, image, *rolled = pl.pallas_call(
            functools.partial(relay_kernel, n_row, n_col, rounds, peaks),
            out_shape=results,
            in_specs=[vmem, hbm, hbm],
            out_specs=(vmem,) * len(results),
            scratch_shapes=[
                *[pltpu.VMEM((padded[0], 6 * depth // PIECES, LANES), jnp.float32)] * PIECES,
                pltpu.VMEM((padded[0], 8 + 2 * depth, LANES), jnp.float32),
                pltpu.VMEM((2, total), jnp.int32),
                pltpu.SMEM((2, total), jnp.int32),
                pltpu.VMEM((codes, LANES), jnp.int32),
                pltpu.SMEM((codes, LANES), jnp.int32),
                pltpu.VMEM((rounds * (rounds - 1) // 2 * peaks, 8, LANES), jnp.int32),
                pltpu.VMEM((2, total, LANES), jnp.int32),
                pltpu.VMEM((4, wells * 8 + 8, LANES), jnp.float32),
                pltpu.VMEM((2 * n_row, wells * 8 + 8, LANES), jnp.float32),
                dma((chunks,)),
                dma((parts,)),
                dma,
                dma,
                dma((3, PIECES)),
                dma((3, PIECES)),
                dma((4, PIECES)),
                dma((4, PIECES)),
                dma((3,)),
                dma((3,)),
                dma((2 * n_row,)),
                dma((2 * n_row,)),
            ],
            compiler_params=params,
            name="gather_beam",
        )(pixels, psf_hbm, res_hbm)
    else:
        codes, skip, rows_done = lookup_codes(n_row, n_col, tile_rows, tile_cols, side, peak_pixels)
        beam, lists, amps, image, *rolled = pl.pallas_call(
            functools.partial(gather_kernel, n_row, n_col, skip, rows_done, rounds, peaks),
            out_shape=results,
            in_specs=[smem, vmem, hbm, hbm],
            out_specs=(vmem,) * len(results),
            scratch_shapes=[
                pltpu.VMEM((2, total), jnp.int32),
                pltpu.SMEM((2, total), jnp.int32),
                pltpu.VMEM((n_dev, groups * 8, LANES), jnp.float32),
                dma((chunks,)),
                dma((parts,)),
                dma,
                dma((n_col,)),
                dma((n_col,)),
                dma((n_col,)),
                dma((n_col,)),
                dma((n_dev,)),
                dma((n_dev,)),
            ],
            compiler_params=params,
            name="gather_beam",
        )(codes, pixels, psf_hbm, res_hbm)

    cleaned, tile_peak, amps = pl.pallas_call(
        functools.partial(subtract_kernel, rounds, peaks, side, tile_rows, tile_cols),
        out_shape=(
            jax.ShapeDtypeStruct((tile_rows, tile_cols), jnp.float32),
            jax.ShapeDtypeStruct((1, 1), jnp.float32),
            jax.ShapeDtypeStruct((rounds, peaks), jnp.float32),
        ),
        in_specs=[vmem] * (4 + parts),
        out_specs=(hbm, vmem, vmem),
        scratch_shapes=[
            pltpu.VMEM((tile_rows, tile_cols), jnp.float32),
            pltpu.SMEM((8, long), jnp.int32),
            pltpu.SMEM((1, total), jnp.float32),
            dma((tile_rows // PAD,)),
            dma,
            dma,
        ],
        compiler_params=pltpu.CompilerParams(vmem_limit_bytes=4 << 20),
        name="subtract",
    )(
        lists,
        image,
        beam.reshape(padded[0] * padded[1], LANES),
        amps,
        *[part.reshape(reach, LANES) for part in rolled],
    )
    return cleaned, tile_peak, amps


def solution(mesh):
    return jax.shard_map(
        functools.partial(local, mesh.shape["row"], mesh.shape["col"]),
        mesh=mesh,
        in_specs=(P("row", "col"), P("col", None), P()),
        out_specs=(P("row", "col"), P("row", "col"), P()),
        check_vma=False,
    )
```

```python
import functools

import jax
import jax.numpy as jnp
from jax import lax
from jax.experimental import pallas as pl
from jax.experimental.pallas import tpu as pltpu
from jax.sharding import PartitionSpec as P

loop_gain = 0.1
LANES = 128
LINE_BIT = 7
CHUNK_BIT = 24
LIST_ROWS = 16
LINE_MASK = (1 << (CHUNK_BIT - LINE_BIT)) - 1
MESH = pl.DeviceIdType.MESH
PAD = 64
AHEAD = 8
STRIDE = 4
FRONT = 32
SPLIT = 2
GROUP = 16
PIECES = 8
LAG = 2
QUEUED = 4
MEET = 4
OWN_STEPS = 2
SCRATCH = 11 << 20


def to_sublanes(line):
    square = lax.broadcasted_iota(jnp.int32, (LANES, LANES), 0) == lax.broadcasted_iota(
        jnp.int32, (LANES, LANES), 1
    )
    pieces = [
        jnp.sum(jnp.where(square, line[:, g : g + LANES], 0.0), axis=1, keepdims=True)
        for g in range(0, line.shape[1], LANES)
    ]
    return jnp.concatenate(pieces, axis=0)


def lane_iota(rows):
    return lax.broadcasted_iota(jnp.int32, (rows, LANES), 1)


def make_lists(row, col, tile_rows, tile_cols, side, pixels, lists, front):
    total = pixels.shape[1]
    spare = lists.shape[1] - total
    blocks = tile_rows // PAD
    pitch = side + 2 * PAD
    top = (pixels[0:1, :] - (row * tile_rows + side // 2)).astype(jnp.float32)
    left = (col * tile_cols + side // 2 - pixels[1:2, :]).astype(jnp.float32)
    inside = (top > -side) & (top < tile_rows) & (left > -tile_cols) & (left < side)
    start = jnp.clip(left.astype(jnp.int32) + tile_cols, 0, side + tile_cols - 1)
    height = jnp.minimum(top + side, tile_rows) - jnp.maximum(top, 0.0)
    height = jnp.where(inside, height, 0.0)
    index = lax.broadcasted_iota(jnp.int32, (1, total), 1).astype(jnp.float32)
    index_down = lax.broadcasted_iota(jnp.int32, (total, 1), 0).astype(jnp.float32)
    slot_at = lax.broadcasted_iota(jnp.int32, (total, total), 1).astype(jnp.float32)
    none, huge = -1.0, 1e9

    tall = index - height * total
    tall_down = to_sublanes(tall)
    rank_down = jnp.sum(jnp.where(tall < tall_down, 1.0, 0.0), axis=1, keepdims=True)
    rank = jnp.sum(jnp.where(tall_down < tall, 1.0, 0.0), axis=0, keepdims=True)
    in_down = to_sublanes(jnp.where(inside, 1.0, 0.0))
    chunk_down = to_sublanes((start >> LINE_BIT).astype(jnp.float32))
    shift_down = to_sublanes((start & (LANES - 1)).astype(jnp.float32))
    top_down = to_sublanes(top)

    def ordered(place_down, down, fill):
        picked = jnp.where(place_down == slot_at, down - fill, 0.0)
        return (jnp.sum(picked, axis=0, keepdims=True) + fill).astype(jnp.int32)

    last = (side + tile_cols - 1) >> LINE_BIT
    front[0:1, :] = jnp.clip(ordered(rank_down, chunk_down, 0.0), 0, last)
    front[1:2, :] = ordered(rank_down, shift_down, 0.0) & (LANES - 1)

    far = 4.0 * tile_rows
    by_top = top * total + index
    by_top_down = to_sublanes(by_top)
    bound = lane_iota(1)
    bound = jnp.where(bound < blocks, bound * PAD + PAD, (bound - blocks) * PAD - side + 1)
    bound = bound.astype(jnp.float32)
    line = 0
    held = FRONT // SPLIT
    for part in range(SPLIT + 1):
        low = part * held
        high = low + held if part < SPLIT else total
        chosen = inside & (rank >= low) & (rank < high)
        chosen_down = jnp.where((rank_down >= low) & (rank_down < high), in_down, 0.0)
        key = jnp.where(chosen, by_top, huge)
        place = jnp.sum(jnp.where(key < by_top_down, 1.0, 0.0), axis=1, keepdims=True)
        place = jnp.where(chosen_down > 0.0, place, none)
        columns = [(top_down, far), None, (index_down, 0.0)]
        if part < SPLIT:
            columns[1] = ((rank_down - low) * (side + PAD) + PAD, PAD)
        else:
            columns[1] = (chunk_down * pitch + PAD, PAD)
            columns.append((shift_down, 0.0))
        for down, fill in columns:
            lists[line : line + 1, :total] = ordered(place, down, fill)
            lists[line : line + 1, total:] = jnp.full((1, spare), int(fill), jnp.int32)
            line += 1
        below = jnp.where(top_down < bound, chosen_down, 0.0)
        count = jnp.sum(below, axis=0, keepdims=True).astype(jnp.int32)
        lists[LIST_ROWS - 1 : LIST_ROWS, part * LANES : (part + 1) * LANES] = count


def spread_pixels(peak_ref, pixel_ref, held_ref, peak_sem):
    rounds, _, peaks = peak_ref.shape
    pltpu.make_async_copy(peak_ref, held_ref, peak_sem).wait()
    for axis in range(2):
        line = [held_ref[r, axis : axis + 1, :] for r in range(rounds)]
        pixel_ref[axis : axis + 1, :] = jnp.concatenate(line, axis=1)


def gather_kernel(
    n_row, n_col, skip, rows_done, rounds, peaks,
    code_ref, peak_ref, psf_ref, res_ref,
    beam, lists, amp_out, image, *rest,
):
    parts = res_ref.shape[1] // LANES
    rolled = rest[: parts * SPLIT]
    (
        held_ref, peak_sem, pixel_ref, front, front_list, table, load_sem, image_sem, front_sem,
        send_sem, recv_sem, pair_send, pair_recv, small_send, small_recv,
    ) = rest[parts * SPLIT :]
    n_dev = n_row * n_col
    side = psf_ref.shape[1]
    chunks = side // LANES
    edge = (beam.shape[0] - chunks) // 2
    depth = side // n_col
    total = rounds * peaks
    groups = total // LANES
    row = lax.axis_index("row")
    col = lax.axis_index("col")
    me = row * n_col + col
    tile_rows, tile_cols = res_ref.shape

    own_loads = [
        pltpu.make_async_copy(
            psf_ref.at[:, pl.ds(c * LANES, LANES)],
            beam.at[edge + c, pl.ds(PAD + col * depth, depth), :],
            load_sem.at[c],
        )
        for c in range(chunks)
    ]
    pltpu.make_async_copy(peak_ref, held_ref, peak_sem).start()
    for copy in own_loads:
        copy.start()
    image_loads = [
        pltpu.make_async_copy(
            res_ref.at[:, pl.ds(u * LANES, LANES)],
            image.at[pl.ds(u * tile_rows, tile_rows), :],
            image_sem.at[u],
        )
        for u in range(parts)
    ]
    for copy in image_loads:
        copy.start()

    barrier = pltpu.get_barrier_semaphore()

    def greet(offset, _):
        other = lax.rem(me + offset, n_dev)
        pl.semaphore_signal(
            barrier, inc=1, device_id=(other // n_col, lax.rem(other, n_col)), device_id_type=MESH
        )
        return 0

    lax.fori_loop(1, n_dev, greet, 0)
    for copy in own_loads:
        copy.wait()
    pl.semaphore_wait(barrier, n_dev - 1)

    def remote(block, device, send, recv):
        region = beam.at[pl.ds(edge, chunks), pl.ds(PAD + block * depth, depth), :]
        return pltpu.make_async_remote_copy(
            src_ref=region,
            dst_ref=region,
            send_sem=send,
            recv_sem=recv,
            device_id=device,
            device_id_type=MESH,
        )

    started = []

    def go(copy):
        copy.start()
        started.append(copy)

    partner = (row, col + 1 - 2 * lax.rem(col, 2))
    chips = n_col // 2

    def hop(step, block):
        target = (row, lax.rem(col + 2 * step, n_col))
        return remote(block, target, send_sem.at[step], recv_sem.at[step])

    def pair(step, block):
        return remote(block, partner, pair_send.at[step], pair_recv.at[step])

    for step in range(1, chips):
        go(hop(step, col))
    go(pair(0, col))

    frame = jnp.zeros((PAD, LANES), jnp.float32)
    for c in range(chunks):
        beam[edge + c, pl.ds(0, PAD), :] = frame
        beam[edge + c, pl.ds(PAD + side, PAD), :] = frame

    def blank(step, _):
        at = pl.multiple_of(step * PAD, PAD)
        for c in list(range(edge)) + list(range(edge + chunks, 2 * edge + chunks)):
            beam[c, pl.ds(at, PAD), :] = frame
        return 0

    lax.fori_loop(0, side // PAD + 2, blank, 0)

    def gap(entry, _):
        at = pl.multiple_of(entry * (side + PAD), PAD)
        for part in rolled:
            part[0, pl.ds(at, PAD), :] = frame
        return 0

    lax.fori_loop(0, FRONT // SPLIT + 1, gap, 0)
    image[pl.ds(parts * tile_rows, 8), :] = jnp.zeros((8, LANES), jnp.float32)
    spread_pixels(peak_ref, pixel_ref, held_ref, peak_sem)
    make_lists(row, col, tile_rows, tile_cols, side, pixel_ref, lists, front)
    front_copy = pltpu.make_async_copy(front, front_list, front_sem)
    front_copy.start()

    def pick(position, carry):
        lane = lax.broadcasted_iota(jnp.int32, (8, LANES), 1)
        code = code_ref[len(rows_done) * total + position]
        which = position & (LANES - 1)
        line = image[pl.ds(code >> LINE_BIT, 1), :]
        moved = pltpu.roll(jnp.broadcast_to(line, (8, LANES)), code & (LANES - 1), 1)
        return jnp.where(lane == which, moved, carry)

    for copy in image_loads:
        copy.wait()
    zero = jnp.zeros((8, LANES), jnp.float32)
    sublane = lax.broadcasted_iota(jnp.int32, (8, LANES), 0)
    picked = []
    for g in range(groups):
        found = lax.fori_loop(g * LANES, (g + 1) * LANES, pick, zero, unroll=32)
        picked.append(jnp.where(sublane == len(rows_done), found, 0.0))
    front_copy.wait()

    band = side // 8
    unit = band // PIECES

    def roll_piece(piece):
        def several(part, step, _):
            for u in range(GROUP):
                entry = step * GROUP + u
                spot = part * (FRONT // SPLIT) + entry
                chunk, shift = front_list[0, spot], front_list[1, spot]
                turn = (LANES - shift) & (LANES - 1)
                keep = lane_iota(unit) >= shift
                for b in range(8):
                    at = b * band + piece * unit
                    cells = [beam[chunk + q, pl.ds(PAD + at, unit), :] for q in range(parts + 1)]
                    goal = pl.multiple_of(entry * (side + PAD) + PAD + at, 8)
                    for q in range(parts):
                        window = jnp.where(keep, cells[q], cells[q + 1])
                        rolled[q * SPLIT + part][0, pl.ds(goal, unit), :] = pltpu.roll(window, turn, 1)
            return 0

        for part in range(SPLIT):
            trips = FRONT // SPLIT // GROUP
            lax.fori_loop(0, trips, functools.partial(several, part), 0)

    for step in range(1, chips):
        source = lax.rem(col - 2 * step + n_col, n_col)
        hop(step, source).wait_recv()
        go(pair(step, source))
    for step in range(chips):
        source = lax.rem(partner[1] - 2 * step + n_col, n_col)
        pair(step, source).wait_recv()

    for g in range(groups):
        active = [(t, need) for t, need in enumerate(rows_done) if need > g * LANES]
        bounds = sorted({min(need, (g + 1) * LANES) for _, need in active})
        carry = zero
        start = g * LANES
        for stop in bounds:
            live = [t for t, need in active if min(need, (g + 1) * LANES) >= stop]

            def look(position, acc):
                lane = lax.broadcasted_iota(jnp.int32, (8, LANES), 1)
                here = lane == (position & (LANES - 1))
                for t in live:
                    code = code_ref[t * total + position]
                    line = beam[code >> CHUNK_BIT, pl.ds((code >> LINE_BIT) & LINE_MASK, 1), :]
                    moved = pltpu.roll(jnp.broadcast_to(line, (8, LANES)), code & (LANES - 1), 1)
                    acc = jnp.where(here & (sublane == t), moved, acc)
                return acc

            carry = lax.fori_loop(start, stop, look, carry, unroll=16)
            start = stop
        table[me, pl.ds(g * 8, 8), :] = carry + picked[g]

    def small(offset, target, slot):
        return pltpu.make_async_remote_copy(
            src_ref=table.at[slot],
            dst_ref=table.at[slot],
            send_sem=small_send.at[offset],
            recv_sem=small_recv.at[offset],
            device_id=(target // n_col, lax.rem(target, n_col)),
            device_id_type=MESH,
        )

    def spread(offset, _):
        small(offset, lax.rem(me + offset, n_dev), me).start()
        return 0

    lax.fori_loop(1, n_dev, spread, 0)

    def every(piece, _):
        roll_piece(piece)
        return 0

    lax.fori_loop(0, PIECES, every, 0)
    for copy in started:
        copy.wait_send()

    def collect(offset, _):
        other = lax.rem(me - offset + n_dev, n_dev)
        small(offset, other, other).wait_recv()
        small(offset, other, me).wait_send()
        return 0

    lax.fori_loop(1, n_dev, collect, 0)

    values = []
    for g in range(groups):
        part = table[:, g * 8 + len(rows_done), :]
        values.append(jnp.sum(part, axis=0, keepdims=True))
    lane = lax.broadcasted_iota(jnp.int32, (1, LANES), 1)
    amps = [jnp.zeros((1, LANES), jnp.float32) for _ in range(groups)]
    piece = min(n_dev, peaks)
    for r in range(rounds):
        g_here = r * peaks // LANES
        lane_here = r * peaks % LANES
        taken = jnp.zeros((1, LANES), jnp.float32)
        if r:
            for first in range(r * peaks, (r + 1) * peaks, piece):
                device, slot = first % n_dev, first // n_dev - skip
                dots = jnp.zeros((piece, LANES), jnp.float32)
                for g in range((r * peaks + LANES - 1) // LANES):
                    rows = table[device : device + piece, g * 8 + slot, :]
                    dots = dots + rows * amps[g]
                sums = jnp.sum(dots, axis=1, keepdims=True)
                spot = lax.broadcasted_iota(jnp.int32, (piece, LANES), 0) + first % LANES
                diag = spot == lax.broadcasted_iota(jnp.int32, (piece, LANES), 1)
                taken = taken + jnp.sum(jnp.where(diag, sums, 0.0), axis=0, keepdims=True)
        fresh = loop_gain * (values[g_here] - taken)
        mine = (lane >= lane_here) & (lane < lane_here + peaks)
        amps[g_here] = jnp.where(mine, fresh, amps[g_here])

    for g in range(groups):
        amp_out[0:1, g * LANES : (g + 1) * LANES] = amps[g]


def relay_kernel(
    n_row, n_col, rounds, peaks,
    peak_ref, psf_ref, res_ref,
    beam, lists, amp_out, image, *rest,
):
    parts = res_ref.shape[1] // LANES
    rolled = rest[: parts * SPLIT]
    stage = rest[parts * SPLIT : parts * SPLIT + 2 * PIECES]
    (
        quarter, held_ref, peak_sem, pixel_ref, front, front_list, code_line, code_list, turns, down, plane, table,
        load_sem, image_sem, front_sem, code_sem, send_sem, recv_sem, pair_send, pair_recv,
        plane_send, plane_recv, line_send, line_recv,
    ) = rest[parts * SPLIT + 2 * PIECES :]
    side = psf_ref.shape[1]
    chunks = side // LANES
    edge = parts
    depth = side // n_col
    total = rounds * peaks
    groups = total // LANES
    tile_rows, tile_cols = res_ref.shape
    strip = depth // PIECES
    row = lax.axis_index("row")
    col = lax.axis_index("col")
    core = lax.rem(col, 2)
    base = col - core
    flip = lax.rem(row, 2)
    near = col + 2 - 4 * lax.rem(col // 2, 2)
    far = col + 4 - 8 * (col // 4)
    across = near + far - col
    first = near + flip * (far - near)
    second = far + flip * (near - far)
    partner = (row, base + 1 - core)
    layer = (row + 1 - 2 * flip, col)
    place = row * 2 + core
    spots = 2 * n_row

    def lined(other):
        return (other // 2, base + lax.rem(other, 2))

    own_loads = [
        pltpu.make_async_copy(
            psf_ref.at[:, pl.ds(c * LANES, LANES)],
            quarter.at[edge + c, pl.ds(8 + core * depth, depth), :],
            load_sem.at[c],
        )
        for c in range(chunks)
    ]
    pltpu.make_async_copy(peak_ref, held_ref, peak_sem).start()
    for copy in own_loads:
        copy.start()
    image_loads = [
        pltpu.make_async_copy(
            res_ref.at[:, pl.ds(u * LANES, LANES)],
            image.at[pl.ds(u * tile_rows, tile_rows), :],
            image_sem.at[u],
        )
        for u in range(parts)
    ]
    for copy in image_loads:
        copy.start()

    barrier = pltpu.get_barrier_semaphore()
    for device in [(row, near), (row, far), (row, across)] + [
        lined(lax.rem(place + offset, spots)) for offset in range(1, spots)
    ]:
        pl.semaphore_signal(barrier, inc=1, device_id=device, device_id_type=MESH)

    rim = list(range(edge)) + list(range(edge + chunks, 2 * edge + chunks))
    for c in range(2 * edge + chunks):
        quarter[c, 0:8, :] = jnp.zeros((8, LANES), jnp.float32)
    for c in rim:
        quarter[c, 8:, :] = jnp.zeros((2 * depth, LANES), jnp.float32)
        for held in stage:
            held[c, :, :] = jnp.zeros(held.shape[1:], jnp.float32)
    image[pl.ds(parts * tile_rows, 8), :] = jnp.zeros((8, LANES), jnp.float32)

    spread_pixels(peak_ref, pixel_ref, held_ref, peak_sem)
    lane = lane_iota(1)
    sublane = lax.broadcasted_iota(jnp.int32, (8, LANES), 0)
    across_lane = lane_iota(8)
    spans, turned = [], []
    flat_rows = quarter.shape[1]
    for axis in range(2):
        line = to_sublanes(pixel_ref[axis : axis + 1, :].astype(jnp.float32))
        down[axis, :, :] = jnp.broadcast_to(line.astype(jnp.int32), (total, LANES))
    for r in range(1, rounds):
        goal_row = down[0, pl.ds(r * peaks + place * 8, 8), :]
        goal_col = down[1, pl.ds(r * peaks + place * 8, 8), :]
        for g in range((r * peaks + LANES - 1) // LANES):
            cut = slice(g * LANES, (g + 1) * LANES)
            di = goal_row - pixel_ref[0:1, cut] + (side // 2 - base * depth)
            dj = goal_col - pixel_ref[1:2, cut] + side // 2
            valid = (di >= 0) & (di < 2 * depth) & (dj >= 0) & (dj < side)
            valid = valid & (lane + g * LANES < r * peaks)
            code = ((dj >> LINE_BIT) + edge) * flat_rows + di + 8
            at = ((r - 1) * groups + g) * 8
            code_line[at : at + 8, :] = jnp.where(valid, code, 8) - sublane
            spans.append((r, g, len(turned), jnp.where(valid, dj & (LANES - 1), 0)))
            turned.extend(range(min(LANES, r * peaks - g * LANES)))
    tail = (rounds - 1) * groups * 8
    for g in range(groups):
        cut = slice(g * LANES, (g + 1) * LANES)
        lr = pixel_ref[0:1, cut] - row * tile_rows
        lc = pixel_ref[1:2, cut] - col * tile_cols
        own = (lr >= 0) & (lr < tile_rows) & (lc >= 0) & (lc < tile_cols)
        flat = jnp.where(own, (lc >> LINE_BIT) * tile_rows + lr, parts * tile_rows)
        code = (flat << LINE_BIT) + ((lane - lc) & (LANES - 1))
        code_line[tail + g : tail + g + 1, :] = code
    code_copy = pltpu.make_async_copy(code_line, code_list, code_sem)
    code_copy.start()

    for r, g, offset, column in spans:

        def splat(at, _):
            turns[offset + at, :, :] = jnp.take_along_axis(
                column, jnp.full((8, LANES), at, jnp.int32), axis=1
            )
            return 0

        lax.fori_loop(0, min(LANES, r * peaks - g * LANES), splat, 0, unroll=64)
    for copy in own_loads:
        copy.wait()
    pl.semaphore_wait(barrier, 3 + spots - 1)

    started = []

    def remote(src, dst, device, send, recv):
        return pltpu.make_async_remote_copy(
            src_ref=src, dst_ref=dst, send_sem=send, recv_sem=recv,
            device_id=device, device_id_type=MESH,
        )

    def go(copy):
        copy.start()
        started.append(copy)

    def spot_of(p, kind, side_of):
        if kind == 0:
            return stage[p], pl.ds(side_of * strip, strip)
        return stage[PIECES + p], pl.ds((kind * 2 - 2 + side_of) * strip, strip)

    def slot(p, kind, side_of):
        held, rows = spot_of(p, kind, side_of)
        return held.at[pl.ds(edge, chunks), rows, :]

    def mine(p):
        return quarter.at[pl.ds(edge, chunks), pl.ds(8 + core * depth + p * strip, strip), :]

    def direct(p):
        return remote(
            mine(p), slot(p, 0, core), (row, first), send_sem.at[0, p], recv_sem.at[0, p]
        )

    def relay(p):
        return remote(
            slot(p, 0, core), slot(p, 1, core), (row, second), send_sem.at[1, p], recv_sem.at[1, p]
        )

    def lift(p):
        return remote(
            slot(p, 0, core), slot(p, 2, core), layer, send_sem.at[2, p], recv_sem.at[2, p]
        )

    def pair(kind, p, side_of):
        at = slot(p, kind, side_of)
        return remote(at, at, partner, pair_send.at[kind, p], pair_recv.at[kind, p])

    def pair_own(side_of):
        at = quarter.at[pl.ds(edge, chunks), pl.ds(8 + side_of * depth, depth), :]
        return remote(at, at, partner, pair_send.at[3, 0], pair_recv.at[3, 0])

    go(pair_own(core))
    for p in range(QUEUED):
        go(direct(p))

    code_copy.wait()
    for copy in image_loads:
        copy.wait()

    def fetch(line, code):
        return pltpu.roll(jnp.broadcast_to(line, (8, LANES)), code & (LANES - 1), 1)

    picked = jnp.zeros((8, LANES), jnp.float32)
    for g in range(groups):

        def pick(at, carry):
            hit = (across_lane == at) & (sublane == g)
            code = code_list[tail + g, at]
            return jnp.where(hit, fetch(image[pl.ds(code >> LINE_BIT, 1), :], code), carry)

        picked = lax.fori_loop(0, LANES, pick, picked, unroll=32)

    wells = [(r, g, offset) for r, g, offset, _ in spans]
    flat_quarter = quarter.reshape((2 * edge + chunks) * flat_rows, LANES)

    def look(begin, end, found):
        g = begin // LANES
        live = [w for w, (r, h, _) in enumerate(wells) if h == g and r * peaks > begin]

        def one(at, held):
            held = list(held)
            here = across_lane == at
            for w in live:
                r, _, offset = wells[w]
                lines = jnp.zeros((8, LANES), jnp.float32)
                for i in range(8):
                    code = code_list[((r - 1) * groups + g) * 8 + i, at]
                    lines = jnp.where(sublane == i, flat_quarter[pl.ds(code, 8), :], lines)
                value = jnp.take_along_axis(lines, turns[offset + at, :, :], axis=1)
                held[w] = jnp.where(here, value, held[w])
            return tuple(held)

        return lax.fori_loop(begin - g * LANES, end - g * LANES, one, found, unroll=16)

    starts = [block * depth for block in (first - core, across - core, second - core)]

    def cell(strip_of, chunk):
        kind, other, piece = strip_of
        if kind is None:
            return quarter[chunk, pl.ds(8 + other * depth + piece * strip, strip), :]
        held, rows = spot_of(piece, kind, other)
        return held[chunk, rows, :]

    def row_of(strip_of):
        kind, other, piece = strip_of
        start = base * depth if kind is None else starts[kind]
        return start + other * depth + piece * strip

    def roll_strips(strips):
        for strip_of in strips:
            at = pl.multiple_of(PAD + row_of(strip_of), 8)
            for c in range(chunks):
                beam[edge + c, pl.ds(at, strip), :] = cell(strip_of, edge + c)

        def several(part, step, _):
            for u in range(GROUP):
                entry = step * GROUP + u
                spot = part * (FRONT // SPLIT) + entry
                chunk, shift = front_list[0, spot], front_list[1, spot]
                turn = (LANES - shift) & (LANES - 1)
                keep = lane_iota(strip) >= shift
                for strip_of in strips:
                    cells = [cell(strip_of, chunk + q) for q in range(parts + 1)]
                    goal = entry * (side + PAD) + PAD + row_of(strip_of)
                    goal = pl.multiple_of(goal, 8)
                    for q in range(parts):
                        window = jnp.where(keep, cells[q], cells[q + 1])
                        rolled[q * SPLIT + part][0, pl.ds(goal, strip), :] = pltpu.roll(
                            window, turn, 1
                        )
            return 0

        for part in range(SPLIT):
            trips = FRONT // SPLIT // GROUP
            lax.fori_loop(0, trips, functools.partial(several, part), 0)

    def swap(j):
        device = (row, (near, far, across)[j])
        return remote(
            plane.at[0], plane.at[1 + j], device, plane_send.at[j], plane_recv.at[j]
        )

    def spread(offset, owner):
        return remote(
            table.at[owner], table.at[owner], lined(lax.rem(place + offset, spots)),
            line_send.at[offset], line_recv.at[offset],
        )

    found = tuple(jnp.zeros((8, LANES), jnp.float32) for _ in wells)
    frame = jnp.zeros((PAD, LANES), jnp.float32)
    pair_own(1 - core).wait_recv()
    for begin in range(0, (rounds - 1) * peaks, peaks):
        found = look(begin, begin + peaks, found)
    for w, part in enumerate(found):
        plane[0, w * 8 : w * 8 + 8, :] = part
    plane[0, len(wells) * 8 :, :] = picked
    for j in range(3):
        go(swap(j))
    for p in range(PIECES + LAG):
        if p < PIECES:
            direct(p).wait_recv()
            if p + QUEUED < PIECES:
                go(direct(p + QUEUED))
            go(relay(p))
            go(lift(p))
            go(pair(0, p, core))
        if p >= LAG:
            q = p - LAG
            relay(q).wait_recv()
            go(pair(1, q, core))
            lift(q).wait_recv()
            go(pair(2, q, core))
        if p == 0:
            make_lists(row, col, tile_rows, tile_cols, side, pixel_ref, lists, front)
            front_copy = pltpu.make_async_copy(front, front_list, front_sem)
            front_copy.start()
        if p == 1:
            for c in range(chunks):
                beam[edge + c, pl.ds(0, PAD), :] = frame
                beam[edge + c, pl.ds(PAD + side, PAD), :] = frame

            def blank(step, _):
                at = pl.multiple_of(step * PAD, PAD)
                for c in rim:
                    beam[c, pl.ds(at, PAD), :] = frame
                return 0

            lax.fori_loop(0, side // PAD + 2, blank, 0)

            def gap(entry, _):
                at = pl.multiple_of(entry * (side + PAD), PAD)
                for part in rolled:
                    part[0, pl.ds(at, PAD), :] = frame
                return 0

            lax.fori_loop(0, FRONT // SPLIT + 1, gap, 0)
            front_copy.wait()
        if p == MEET:
            for j in range(3):
                swap(j).wait_recv()
            table[place, :, :] = plane[0] + plane[1] + plane[2] + plane[3]
            for offset in range(1, spots):
                go(spread(offset, place))
        strips = []
        if p > 0 and p <= PIECES:
            pair(0, p - 1, 1 - core).wait_recv()
            strips += [(0, other, p - 1) for other in range(2)]
        if p > LAG:
            q = p - LAG - 1
            for kind in range(1, 3):
                pair(kind, q, 1 - core).wait_recv()
                strips += [(kind, other, q) for other in range(2)]
        if strips:
            roll_strips(strips)
        if 0 < p <= OWN_STEPS:
            count = PIECES // OWN_STEPS
            pieces = range((p - 1) * count, p * count)
            roll_strips([(None, other, piece) for piece in pieces for other in range(2)])
    for offset in range(1, spots):
        spread(offset, lax.rem(place - offset + spots, spots)).wait_recv()

    values = sum(table[z, len(wells) * 8 :, :] for z in range(spots))
    values = [values[g : g + 1, :] for g in range(groups)]
    amps = [jnp.zeros((1, LANES), jnp.float32) for _ in range(groups)]
    for r in range(rounds):
        g_here, lane_here = r * peaks // LANES, r * peaks % LANES
        taken = jnp.zeros((1, LANES), jnp.float32)
        if r:
            dots = jnp.zeros((peaks, LANES), jnp.float32)
            for w, (s, g, _) in enumerate(wells):
                if s == r:
                    rows = jnp.concatenate(
                        [table[z, w * 8 : w * 8 + 8, :] for z in range(spots)], axis=0
                    )
                    dots = dots + rows * amps[g]
            sums = jnp.sum(dots, axis=1, keepdims=True)
            spot = lax.broadcasted_iota(jnp.int32, (peaks, LANES), 0) + lane_here
            taken = jnp.sum(
                jnp.where(spot == lane_iota(peaks), sums, 0.0), axis=0, keepdims=True
            )
        fresh = loop_gain * (values[g_here] - taken)
        here = (lane >= lane_here) & (lane < lane_here + peaks)
        amps[g_here] = jnp.where(here, fresh, amps[g_here])
    for g in range(groups):
        amp_out[0:1, g * LANES : (g + 1) * LANES] = amps[g]
    for kind in range(1, 3):
        pair(kind, PIECES - 1, 1 - core).wait_recv()
    roll_strips([(kind, other, PIECES - 1) for kind in range(1, 3) for other in range(2)])
    for copy in started:
        copy.wait_send()


def subtract_kernel(
    rounds, peaks, side,
    tile_rows, tile_cols, lists_ref, image_ref, beam_ref, amps_ref, *rest,
):
    pitch_rows = side + 2 * PAD
    parts = tile_cols // LANES
    blocks = tile_rows // PAD
    rolled = rest[: parts * SPLIT]
    (
        clean_ref, peak_ref, amp_ref,
        image, lists, amp_list, store_sem, list_sem, amp_sem,
    ) = rest[parts * SPLIT :]

    copies = [
        pltpu.make_async_copy(lists_ref, lists, list_sem),
        pltpu.make_async_copy(amps_ref, amp_list, amp_sem),
    ]
    for copy in copies:
        copy.start()
    for r in range(rounds):
        amp_ref[r : r + 1, :] = amps_ref[0:1, r * peaks : (r + 1) * peaks]
    for copy in copies:
        copy.wait()

    def store(block):
        at = pl.multiple_of(block * PAD, PAD)
        return pltpu.make_async_copy(
            image.at[pl.ds(at, PAD), :], clean_ref.at[pl.ds(at, PAD), :], store_sem.at[block]
        )

    lanes = lane_iota(PAD)

    def settle(block, best):
        at = pl.multiple_of(block * PAD, PAD)

        starts = [lists[LIST_ROWS - 1, k * LANES + blocks + block] for k in range(SPLIT + 1)]
        ends = [lists[LIST_ROWS - 1, k * LANES + block] for k in range(SPLIT + 1)]
        later = starts[SPLIT]

        def still(k, entry, held):
            first = lists[3 * k + 1, entry] + jnp.maximum(at - lists[3 * k, entry], -PAD)
            amplitude = amp_list[0, lists[3 * k + 2, entry]]
            return [
                held[q] - amplitude * rolled[q * SPLIT + k][pl.ds(first, PAD), :]
                for q in range(parts)
            ]

        def turning(entry, held):
            line = 3 * SPLIT
            first = lists[line + 1, entry] + jnp.maximum(at - lists[line, entry], -PAD)
            amplitude = amp_list[0, lists[line + 2, entry]]
            shift = lists[line + 3, entry]
            turn = (LANES - shift) & (LANES - 1)
            keep = lanes >= shift
            cells = [beam_ref[pl.ds(first + q * pitch_rows, PAD), :] for q in range(parts + 1)]
            moved = [
                pltpu.roll(jnp.where(keep, cells[q], cells[q + 1]), turn, 1) for q in range(parts)
            ]
            return [held[q] - amplitude * moved[q] for q in range(parts)]

        def both(step, held):
            held = list(held)
            for k in range(SPLIT):
                for u in range(STRIDE):
                    held = still(k, starts[k] + step * STRIDE + u, held)
            for u in range(AHEAD):
                held = turning(later + step * AHEAD + u, held)
            return tuple(held)

        def rest_of(k, step, held):
            held = list(held)
            for u in range(STRIDE):
                held = still(k, starts[k] + step * STRIDE + u, held)
            return tuple(held)

        held = tuple(image_ref[pl.ds(q * tile_rows + at, PAD), :] for q in range(parts))
        trips = (ends[SPLIT] - later + AHEAD - 1) // AHEAD
        held = lax.fori_loop(0, trips, both, held)
        for k in range(SPLIT):
            more = (ends[k] - starts[k] + STRIDE - 1) // STRIDE
            held = lax.fori_loop(trips, more, functools.partial(rest_of, k), held)
        for q in range(parts):
            image[pl.ds(at, PAD), q * LANES : (q + 1) * LANES] = held[q]
            for i in range(0, PAD, 8):
                best = jnp.maximum(best, jnp.abs(held[q][i : i + 8, :]))
        store(block).start()
        return best

    best = jnp.zeros((8, LANES), jnp.float32)
    best = lax.fori_loop(0, blocks, settle, best)
    peak_ref[...] = jnp.max(jnp.max(best, axis=0, keepdims=True), axis=1, keepdims=True)

    def finish(block, _):
        store(block).wait()
        return 0

    lax.fori_loop(0, blocks, finish, 0)


def lookup_codes(n_row, n_col, tile_rows, tile_cols, side, peak_pixels):
    n_dev = n_row * n_col
    chunks = side // LANES
    half_width = side // 2
    rounds, peaks, _ = peak_pixels.shape
    total = rounds * peaks
    row_base = lax.axis_index("row") * tile_rows
    col_base = lax.axis_index("col") * tile_cols
    me = lax.axis_index("row") * n_col + lax.axis_index("col")
    parts = tile_cols // LANES

    per_device = total // n_dev
    skip = peaks // n_dev if peaks % n_dev == 0 else 0
    coeff_rows = per_device - skip
    if peaks % n_dev == 0:
        rows_done = tuple((t * n_dev // peaks) * peaks for t in range(skip, per_device))
    else:
        rows_done = (total,) * coeff_rows

    flat = peak_pixels.reshape(total, 2)
    prow, pcol = flat[:, 0], flat[:, 1]
    index = jnp.arange(total, dtype=jnp.int32)
    slots = lax.dynamic_slice(
        peak_pixels.reshape(per_device, n_dev, 2), (skip, me, 0), (coeff_rows, 1, 2)
    )
    target = me + n_dev * (jnp.arange(coeff_rows, dtype=jnp.int32) + skip)
    di = slots[:, :, 0] - prow[None, :] + half_width
    dj = slots[:, :, 1] - pcol[None, :] + half_width
    earlier = (index // peaks)[None, :] < (target // peaks)[:, None]
    valid = (di >= 0) & (di < side) & (dj >= 0) & (dj < side) & earlier
    look = (dj // LANES + parts << CHUNK_BIT) + (di + PAD << LINE_BIT)
    look = jnp.where(valid, look + (index[None, :] - dj) % LANES, 0)
    lr, lc = prow - row_base, pcol - col_base
    own = (lr >= 0) & (lr < tile_rows) & (lc >= 0) & (lc < tile_cols)
    pick = (lc // LANES * tile_rows + lr << LINE_BIT) + (index - lc) % LANES
    pick = jnp.where(own, pick, parts * tile_rows << LINE_BIT)
    codes = jnp.stack([*look, pick]).reshape(-1)
    return codes, skip, rows_done


def local(n_row, n_col, residual, point_spread, peak_pixels):
    n_dev = n_row * n_col
    tile_rows, tile_cols = residual.shape
    side = point_spread.shape[1]
    chunks = side // LANES
    rounds, peaks, _ = peak_pixels.shape
    total = rounds * peaks
    groups = total // LANES
    parts = tile_cols // LANES
    pixels = jnp.transpose(peak_pixels, (0, 2, 1))
    pixels = pltpu.with_memory_space_constraint(pixels, pltpu.HBM)

    smem = pl.BlockSpec(memory_space=pltpu.SMEM)
    vmem = pl.BlockSpec(memory_space=pltpu.VMEM)
    hbm = pl.BlockSpec(memory_space=pltpu.HBM)
    dma = pltpu.SemaphoreType.DMA
    padded = (chunks + 2 * parts, side + 2 * PAD, LANES)
    long = total + LANES
    reach = FRONT // SPLIT * (side + PAD) + PAD
    psf_hbm = pltpu.with_memory_space_constraint(point_spread, pltpu.HBM)
    res_hbm = pltpu.with_memory_space_constraint(residual, pltpu.HBM)
    results = (
        pltpu.VMEM(padded, jnp.float32),
        pltpu.VMEM((LIST_ROWS, long), jnp.int32),
        pltpu.VMEM((1, total), jnp.float32),
        pltpu.VMEM((parts * tile_rows + 8, LANES), jnp.float32),
        *[pltpu.VMEM((1, reach, LANES), jnp.float32)] * (parts * SPLIT),
    )
    params = pltpu.CompilerParams(
        collective_id=0, has_side_effects=True, vmem_limit_bytes=SCRATCH
    )
    if (n_row, n_col) == (4, 8) and (rounds, peaks) == (4, 64):
        depth = side // n_col
        wells = sum((r * peaks + LANES - 1) // LANES for r in range(1, rounds))
        codes = (rounds - 1) * groups * 8 + 8
        beam, lists, amps, image, *rolled = pl.pallas_call(
            functools.partial(relay_kernel, n_row, n_col, rounds, peaks),
            out_shape=results,
            in_specs=[hbm, hbm, hbm],
            out_specs=(vmem,) * len(results),
            scratch_shapes=[
                *[pltpu.VMEM((padded[0], 2 * depth // PIECES, LANES), jnp.float32)] * PIECES,
                *[pltpu.VMEM((padded[0], 4 * depth // PIECES, LANES), jnp.float32)] * PIECES,
                pltpu.VMEM((padded[0], 8 + 2 * depth, LANES), jnp.float32),
                pltpu.VMEM((rounds, 2, peaks), jnp.int32),
                dma,
                pltpu.VMEM((2, total), jnp.int32),
                pltpu.VMEM((2, total), jnp.int32),
                pltpu.SMEM((2, total), jnp.int32),
                pltpu.VMEM((codes, LANES), jnp.int32),
                pltpu.SMEM((codes, LANES), jnp.int32),
                pltpu.VMEM((rounds * (rounds - 1) // 2 * peaks, 8, LANES), jnp.int32),
                pltpu.VMEM((2, total, LANES), jnp.int32),
                pltpu.VMEM((4, wells * 8 + 8, LANES), jnp.float32),
                pltpu.VMEM((2 * n_row, wells * 8 + 8, LANES), jnp.float32),
                dma((chunks,)),
                dma((parts,)),
                dma,
                dma,
                dma((3, PIECES)),
                dma((3, PIECES)),
                dma((4, PIECES)),
                dma((4, PIECES)),
                dma((3,)),
                dma((3,)),
                dma((2 * n_row,)),
                dma((2 * n_row,)),
            ],
            compiler_params=params,
            name="gather_beam",
        )(pixels, psf_hbm, res_hbm)
    else:
        codes, skip, rows_done = lookup_codes(n_row, n_col, tile_rows, tile_cols, side, peak_pixels)
        beam, lists, amps, image, *rolled = pl.pallas_call(
            functools.partial(gather_kernel, n_row, n_col, skip, rows_done, rounds, peaks),
            out_shape=results,
            in_specs=[smem, hbm, hbm, hbm],
            out_specs=(vmem,) * len(results),
            scratch_shapes=[
                pltpu.VMEM((rounds, 2, peaks), jnp.int32),
                dma,
                pltpu.VMEM((2, total), jnp.int32),
                pltpu.VMEM((2, total), jnp.int32),
                pltpu.SMEM((2, total), jnp.int32),
                pltpu.VMEM((n_dev, groups * 8, LANES), jnp.float32),
                dma((chunks,)),
                dma((parts,)),
                dma,
                dma((n_col,)),
                dma((n_col,)),
                dma((n_col,)),
                dma((n_col,)),
                dma((n_dev,)),
                dma((n_dev,)),
            ],
            compiler_params=params,
            name="gather_beam",
        )(codes, pixels, psf_hbm, res_hbm)

    cleaned, tile_peak, amps = pl.pallas_call(
        functools.partial(subtract_kernel, rounds, peaks, side, tile_rows, tile_cols),
        out_shape=(
            jax.ShapeDtypeStruct((tile_rows, tile_cols), jnp.float32),
            jax.ShapeDtypeStruct((1, 1), jnp.float32),
            jax.ShapeDtypeStruct((rounds, peaks), jnp.float32),
        ),
        in_specs=[vmem] * (4 + parts * SPLIT),
        out_specs=(hbm, vmem, vmem),
        scratch_shapes=[
            pltpu.VMEM((tile_rows, tile_cols), jnp.float32),
            pltpu.SMEM((LIST_ROWS, long), jnp.int32),
            pltpu.SMEM((1, total), jnp.float32),
            dma((tile_rows // PAD,)),
            dma,
            dma,
        ],
        compiler_params=pltpu.CompilerParams(vmem_limit_bytes=4 << 20),
        name="subtract",
    )(
        lists,
        image,
        beam.reshape(padded[0] * padded[1], LANES),
        amps,
        *[part.reshape(reach, LANES) for part in rolled],
    )
    return cleaned, tile_peak, amps


def solution(mesh):
    return jax.shard_map(
        functools.partial(local, mesh.shape["row"], mesh.shape["col"]),
        mesh=mesh,
        in_specs=(P("row", "col"), P("col", None), P()),
        out_specs=(P("row", "col"), P("row", "col"), P()),
        check_vma=False,
    )
```
